32 devices in a mesh: gx: 8 (over z, x), gy: 2 (over y), gz: 2 (over core).
Axes of the slice: x: 2, y: 2, z: 4, core: 2. Of those that a mesh axis runs over, the one named last changes fastest.
Arguments:
- velocity_term: float32 [32, 64, 256], P('gx', 'gy', 'gz'), may hold values from 0.05 to 0.2
- model_step: float32 [32, 64, 256], P('gx', 'gy', 'gz'), may hold values from -6 to 6
- background: bfloat16 [4, 32, 64, 256], P(None, 'gx', 'gy', 'gz'), may hold values from -6 to 6
- receivers: int32 [3, 256], replicated, may hold values from 0 to 255, as said below
- checkpoints: int32 [16], replicated, may hold values from 0 to 3, as said below
Outputs:
- image: float32 [32, 64, 256], P('gx', 'gy', 'gz')
- traces: float32 [16, 256], replicated
- column_image: float32 [32, 64], P('gx', 'gy')
- wavefield: float32 [32, 64, 256], P('gx', 'gy', 'gz')
The draws below stay inside these ranges and needn't reach their ends.
Inputs may be any that keep to these rules, and one draw needn't show every extreme that they name: receivers[0] indexes the first lateral dimension (below 32), receivers[1] the second (below 64), receivers[2] depth (below 256). `checkpoints`: never falling over the time steps, beginning at 0 and ending at 3.
All inputs are finite; a program needn't handle non-finite values.
Results may differ from the reference program's by a relative error of at most 0.0003.
Values sent between devices are 32-bit elements; how exact they have to be, the bound alone decides.
A program may use at most 64 MiB of HBM per device.

```python
import jax
import jax.numpy as jnp
from jax import lax

NT = 16
NCK = 4
RECV = 256
NX = 32
NY = 64
NZ = 256


def draw_receivers(key, part):
    key_x = jax.random.fold_in(key, 11)
    key_y = jax.random.fold_in(key, 12)
    key_z = jax.random.fold_in(key, 13)
    first = jax.random.randint(key_x, (RECV,), 0, NX)
    second = jax.random.randint(key_y, (RECV,), 0, NY)
    third = jax.random.randint(key_z, (RECV,), 0, NZ)
    return jnp.stack([first, second, third]).astype(jnp.int32)


def draw_checkpoints(key, part):
    inner = jax.random.fold_in(key, 21)
    values = jnp.sort(jax.random.randint(inner, (NT,), 0, NCK))
    values = values.at[0].set(0).at[NT - 1].set(NCK - 1)
    return values.astype(jnp.int32)


def block_levels(key, shape, pieces, smallest, top_value):
    gain, own = 1.0, jax.random.fold_in(key, 6)
    for dim, shards_of in pieces:
        steps = jnp.exp(jax.random.uniform(jax.random.fold_in(own, dim), (shards_of,), jnp.float32, smallest / len(pieces), top_value / len(pieces)))
        gain = gain * jnp.repeat(steps, shape[dim] // shards_of).reshape([-1 if axis == dim else 1 for axis in range(len(shape))])
    return gain


def centred(rng, dims, width, most, cuts=(), kind=jnp.bfloat16):
    array = width * jax.random.normal(rng, dims, jnp.float32)
    if cuts:
        array = array * block_levels(rng, dims, cuts, -0.22, 0.18)
    return jnp.clip(array, -most, most).astype(kind)


def setup_inputs(seed: int = 0) -> dict:
    seeds = jax.random.split(jax.random.key(seed), 6)
    return {
        "velocity_term": jnp.clip(0.05 + 0.15 * jax.random.uniform(seeds[0], (NX, NY, NZ), jnp.float32) ** block_levels(seeds[0], (NX, NY, NZ), ((0, 8), (1, 2), (2, 2)), -0.2, 0.2), 0.05, 0.2),
        "model_step": centred(seeds[1], (NX, NY, NZ), 1.0, 6.0, ((0, 8), (1, 2), (2, 2)), jnp.float32),
        "background": centred(seeds[2], (NCK, NX, NY, NZ), 1.0, 6.0, ((1, 8), (2, 2), (3, 2))),
        "receivers": draw_receivers(jax.random.fold_in(seeds[5], 71), 0),
        "checkpoints": draw_checkpoints(jax.random.fold_in(seeds[5], 71), 0),
    }


near_coef = 4.0 / 3.0
far_coef = -1.0 / 12.0
center_coef = -2.5


def laplace(field):
    total = 3.0 * center_coef * field
    for dim in (0, 1):
        total = total + near_coef * (jnp.roll(field, 1, dim) + jnp.roll(field, -1, dim))
        total = total + far_coef * (jnp.roll(field, 2, dim) + jnp.roll(field, -2, dim))
    padded = jnp.pad(field, ((0, 0), (0, 0), (2, 2)))
    total = total + near_coef * (padded[:, :, 3:-1] + padded[:, :, 1:-3])
    total = total + far_coef * (padded[:, :, 4:] + padded[:, :, :-4])
    return total


def reference(velocity_term, model_step, background, receivers, checkpoints):
    rec_x = receivers[0]
    rec_y = receivers[1]
    rec_z = receivers[2]
    zeros = jnp.zeros(model_step.shape, jnp.float32)
    previous = zeros
    current = zeros
    samples = []
    for step in range(NT):
        accel = lax.dynamic_index_in_dim(background, checkpoints[step], 0, keepdims=False).astype(jnp.float32)
        following = 2.0 * current - previous + velocity_term * laplace(current) + model_step * accel
        samples.append(following[rec_x, rec_y, rec_z])
        previous = current
        current = following
    traces = jnp.stack(samples)
    wavefield = current
    later_two = zeros
    later = zeros
    image = zeros
    for back in range(NT):
        step = NT - 1 - back
        accel = lax.dynamic_index_in_dim(background, checkpoints[step], 0, keepdims=False).astype(jnp.float32)
        adjoint = 2.0 * later - later_two + laplace(velocity_term * later)
        adjoint = adjoint.at[rec_x, rec_y, rec_z].add(traces[step])
        image = image + adjoint * accel
        later_two = later
        later = adjoint
    column_image = jnp.sum(image, axis=2) / NZ
    return image, traces, column_image, wavefield
```

```python
import functools

import jax
import jax.numpy as jnp
from jax import lax
from jax.experimental import pallas as pl
from jax.experimental.pallas import tpu as pltpu
from jax.sharding import PartitionSpec as P

near_coef = 4.0 / 3.0
far_coef = -1.0 / 12.0
center_coef = -2.5


def with_halo(block, sides, width, periodic):
    for axis, dim in sides:
        count = lax.axis_size(axis)
        forward = [(i, i + 1) for i in range(count - 1)]
        if periodic:
            forward.append((count - 1, 0))
        backward = [(target, source) for source, target in forward]
        low = lax.ppermute(
            lax.slice_in_dim(block, block.shape[dim] - width, None, axis=dim), axis, forward
        )
        high = lax.ppermute(lax.slice_in_dim(block, 0, width, axis=dim), axis, backward)
        block = jnp.concatenate([low, block, high], axis=dim)
    return block


def along(padded, dim):
    count = padded.shape[dim]
    first = lax.slice_in_dim(padded, 3, count - 1, axis=dim) + lax.slice_in_dim(
        padded, 1, count - 3, axis=dim
    )
    second = lax.slice_in_dim(padded, 4, count, axis=dim) + lax.slice_in_dim(
        padded, 0, count - 4, axis=dim
    )
    return near_coef * first + far_coef * second


def laplace(field):
    side = with_halo(field, (("gx", 0), ("gy", 1)), 2, True)
    deep = with_halo(field, (("gz", 2),), 2, False)
    x_pad = side[:, 2:-2, :]
    y_pad = side[2:-2, :, :]
    return 3.0 * center_coef * field + along(x_pad, 0) + along(y_pad, 1) + along(deep, 2)


def sample_row(samples, field, step, clip_x, clip_y, clip_z, inside):
    values = field[clip_x, clip_y, clip_z] * inside
    return lax.dynamic_update_index_in_dim(samples, values, step, 0)


def on_device(velocity_term, model_step, background, receivers, checkpoints):
    size_x, size_y, size_z = model_step.shape
    steps = checkpoints.shape[0]
    local_x = receivers[0] - lax.axis_index("gx") * size_x
    local_y = receivers[1] - lax.axis_index("gy") * size_y
    local_z = receivers[2] - lax.axis_index("gz") * size_z
    inside = (
        (local_x >= 0)
        & (local_x < size_x)
        & (local_y >= 0)
        & (local_y < size_y)
        & (local_z >= 0)
        & (local_z < size_z)
    )
    inside = inside.astype(jnp.float32)
    clip_x = jnp.clip(local_x, 0, size_x - 1)
    clip_y = jnp.clip(local_y, 0, size_y - 1)
    clip_z = jnp.clip(local_z, 0, size_z - 1)
    zeros = jnp.zeros(model_step.shape, jnp.float32)
    record = jnp.zeros((steps, receivers.shape[1]), jnp.float32)

    def forward(step, carry):
        previous, current, samples = carry
        accel = lax.dynamic_index_in_dim(background, checkpoints[step], 0, keepdims=False).astype(
            jnp.float32
        )
        following = 2.0 * current - previous + velocity_term * laplace(current) + model_step * accel
        samples = sample_row(samples, following, step, clip_x, clip_y, clip_z, inside)
        return (current, following, samples)

    previous, current, record = lax.fori_loop(0, steps, forward, (zeros, zeros, record))
    traces = lax.psum(record, ("gx", "gy", "gz"))

    def adjoint_step(back, carry):
        later_two, later, image = carry
        step = steps - 1 - back
        accel = lax.dynamic_index_in_dim(background, checkpoints[step], 0, keepdims=False).astype(
            jnp.float32
        )
        adjoint = 2.0 * later - later_two + laplace(velocity_term * later)
        inject = lax.dynamic_index_in_dim(traces, step, 0, keepdims=False) * inside
        adjoint = adjoint.at[clip_x, clip_y, clip_z].add(inject)
        return (later, adjoint, image + adjoint * accel)

    later_two, later, image = lax.fori_loop(0, steps, adjoint_step, (zeros, zeros, zeros))
    depth_total = size_z * lax.axis_size("gz")
    column_image = lax.psum(jnp.sum(image, axis=2), "gz") / depth_total
    return (image, traces, column_image, current)


MESH = pl.DeviceIdType.MESH
BLOCK = 4
GROUP = 4


def place_of(p, gxs, gys, gzs):
    q, gz = p // gzs, p % gzs
    per = 2 * gys
    zz, w = q // per, q % per
    w = w + (zz % 2) * (per - 1 - 2 * w)
    xx, yy = w // gys, w % gys
    return 2 * zz + xx, yy + xx * (gys - 1 - 2 * yy), gz


def position_of(gx, gy, gz, gxs, gys, gzs):
    per = 2 * gys
    zz, xx = gx // 2, gx % 2
    w = xx * gys + gy + xx * (gys - 1 - 2 * gy)
    w = w + (zz % 2) * (per - 1 - 2 * w)
    return (zz * per + w) * gzs + gz


def lane_roll(a, k):
    return pltpu.roll(a, k % a.shape[-1], a.ndim - 1)


def row_roll(a, k):
    return pltpu.roll(a, k % a.shape[-2], a.ndim - 2)


def quarter_owner(k, gy):
    base = (k % 2) * 2 + k // 2
    return base + gy * (2 - 4 * (k % 2))


class Plane:
    def __init__(self, rows, lanes):
        half = lanes // 2
        lane = lax.broadcasted_iota(jnp.int32, (rows, lanes), 1)
        y = lane % half
        self.half = half
        self.first, self.second = y < 1, y < 2
        self.last, self.before = y >= half - 1, y >= half - 2
        self.even = lane < half
        self.odd_quarter = lane % half >= half // 2

    def swap_quarters(self, a):
        quarter = self.half // 2
        return jnp.where(self.odd_quarter, lane_roll(a, quarter), lane_roll(a, -quarter))

    def join(self, low, high):
        return (
            jnp.where(self.odd_quarter, high, low),
            self.swap_quarters(jnp.where(self.odd_quarter, low, high)),
        )

    def split(self, f0, f1):
        t = self.swap_quarters(f1)
        return jnp.where(self.odd_quarter, t, f0), jnp.where(self.odd_quarter, f0, t)

    def along_y(self, f, r):
        near = lane_roll(jnp.where(self.first, r, f), -1) + lane_roll(jnp.where(self.last, r, f), 1)
        far = lane_roll(jnp.where(self.second, r, f), -2) + lane_roll(jnp.where(self.before, r, f), 2)
        return near, far

    def lateral(self, f):
        r = lane_roll(f, self.half)
        near, far = self.along_y(f, r)
        f0, f1, r0, r1 = f[:, 0], f[:, 1], r[:, 0], r[:, 1]
        near = near + r + jnp.stack(
            [jnp.where(self.even, row_roll(r1, 1), r1), jnp.where(self.even, r0, row_roll(r0, -1))], axis=1
        )
        far = far + jnp.stack([f1 + row_roll(f1, 1), f0 + row_roll(f0, -1)], axis=1)
        return near, far


def chain_kernel(
    dims, v_hbm, m_hbm, bg_hbm, rec_hbm, ck_hbm,
    image_ref, traces_ref, column_ref, wave_ref,
    v_in, m_in, bg_in, rec_in, ck_in,
    stage, landed, vel, src, far, own_bg, hist, adj, wbuf, img, count, part, tr1, tr2,
    back_w, back_i, back_c, in_w, in_i, in_c,
    s_0, s_in, r_in, s_c, r_c, s_f, r_f, s_t, r_t, s_w, r_w, s_i, r_i, s_k, r_k,
):
    gxs, gys, gzs, sx, sy, sz, nck, steps = dims
    n = gxs * gys * gzs
    rows = gxs * gys
    lanes = sx * sy
    nz = sz * gzs // n
    per = sz // nz
    fields = 2 + nck
    gx, gy, gz = lax.axis_index("gx"), lax.axis_index("gy"), lax.axis_index("gz")
    pos = position_of(gx, gy, gz, gxs, gys, gzs)
    my_row = gx * gys + gy
    lo_id = place_of(jnp.maximum(pos - 1, 0), gxs, gys, gzs)
    hi_id = place_of(jnp.minimum(pos + 1, n - 1), gxs, gys, gzs)
    has_lo, has_hi = pos > 0, pos < n - 1
    ext = 3 * nz
    f32 = jnp.float32
    tile = (gxs, lanes)

    def remote(src_ref, dst_ref, ss, rs, where):
        return pltpu.make_async_remote_copy(
            src_ref=src_ref, dst_ref=dst_ref, send_sem=ss, recv_sem=rs, device_id=where, device_id_type=MESH
        )

    barrier = pltpu.get_barrier_semaphore()

    def greet(p, carry):
        @pl.when(p != pos)
        def _():
            pl.semaphore_signal(barrier, inc=1, device_id=place_of(p, gxs, gys, gzs), device_id_type=MESH)
        return carry

    loads = [
        pltpu.make_async_copy(a, b, s_0.at[i])
        for i, (a, b) in enumerate(
            ((v_hbm, v_in), (m_hbm, m_in), (bg_hbm, bg_in), (rec_hbm, rec_in), (ck_hbm, ck_in))
        )
    ]
    for load in loads:
        load.start()
    lax.fori_loop(0, n, greet, 0)

    plane = Plane(gxs, lanes)

    @pl.when(jnp.logical_not(has_lo))
    def _():
        vel[0:nz] = jnp.zeros((nz, 2) + tile, f32)
        for k in range(nck):
            src[k, 0:nz] = jnp.zeros((nz, 2) + tile, f32)
        for t in range(steps):
            hist[t, 0:nz] = jnp.zeros((nz, 2) + tile, f32)
            adj[t, 0:nz] = jnp.zeros((nz, 2) + tile, f32)

    @pl.when(jnp.logical_not(has_hi))
    def _():
        vel[2 * nz :] = jnp.zeros((nz, 2) + tile, f32)
        for k in range(nck):
            src[k, 2 * nz :] = jnp.zeros((nz, 2) + tile, f32)
        for t in range(steps):
            hist[t, 2 * nz :] = jnp.zeros((nz, 2) + tile, f32)
            adj[t, 2 * nz :] = jnp.zeros((nz, 2) + tile, f32)

    for load in loads[:3]:
        load.wait()
    for f in range(fields):
        pieces = []
        for k in range(sx):
            x = quarter_owner(k, gy)
            if f == 0:
                pieces.append(v_in[x])
            elif f == 1:
                pieces.append(m_in[x])
            else:
                pieces.append(bg_in[f - 2, x].astype(f32))
        turned = jnp.concatenate(pieces, axis=0).T
        stage[:, f * nz : (f + 1) * nz, :] = turned.reshape(per, nz, lanes)
    pl.semaphore_wait(barrier, n - 1)

    slab = fields * nz

    def arrival(row):
        return landed.at[pl.ds(pl.multiple_of(row * slab, nz), slab)]

    def scatter_in(c, carry):
        p = gz * per + c

        @pl.when(p != pos)
        def _():
            remote(stage.at[c], arrival(my_row), s_in.at[c], r_in.at[my_row], place_of(p, gxs, gys, gzs)).start()

        @pl.when(p == pos)
        def _():
            landed[pl.ds(pl.multiple_of(my_row * slab, nz), slab), :] = stage[c]

        return carry

    lax.fori_loop(0, per, scatter_in, 0)

    for load in loads[3:]:
        load.wait()
    rec = rec_in[...]
    rx, ry, rz = rec[0:1], rec[1:2], rec[2:3]
    nrec = rec.shape[1]
    rlane = (rx % 2) * (lanes // 2) + ry
    rlocal = rz - (pos - 1) * nz
    zr = jnp.where((rlocal >= 0) & (rlocal < ext), (rlocal * 2 + (rx % sx) // 2) * gxs + rx // sx, -1)
    one_zr = (lax.broadcasted_iota(jnp.int32, (ext * rows, nrec), 0) == zr).astype(f32)
    one_lane = (lax.broadcasted_iota(jnp.int32, (lanes, nrec), 0) == rlane).astype(f32)
    counted = lax.dot_general(
        one_zr.astype(jnp.bfloat16), one_lane.astype(jnp.bfloat16), (((1,), (1,)), ((), ())),
        preferred_element_type=f32,
    )
    count[...] = counted.reshape((ext, 2) + tile)
    img[...] = jnp.zeros_like(img)

    owner = pos // per

    def wait_in(row, carry):
        sender = row // gys, row % gys, owner

        @pl.when((row != my_row) | (owner != gz))
        def _():
            remote(stage.at[0], arrival(row), s_in.at[0], r_in.at[row], sender).wait_recv()

        return carry

    lax.fori_loop(0, rows, wait_in, 0)

    def gathered(f, z):
        low = landed[pl.ds(f * nz + z, gxs, stride=gys * slab), :]
        high = landed[pl.ds(slab + f * nz + z, gxs, stride=gys * slab), :]
        return plane.join(low, high)

    for z in range(nz):
        vs = gathered(0, z)
        ms = gathered(1, z)
        for c in range(2):
            vel[nz + z, c] = far_coef * vs[c]
        for k in range(nck):
            accel = gathered(2 + k, z)
            for c in range(2):
                own_bg[k, z, c] = accel[c]
                src[k, nz + z, c] = ms[c] * accel[c]

    halo = 2 * BLOCK
    soon, rest = halo // 4, halo // 2

    def pairs(make):
        return make(0, lo_id), make(1, hi_id)

    def ranges(side, near_at, size):
        at = nz - near_at - size if side else near_at
        return pl.ds(nz + at, size), pl.ds(at if side else 2 * nz + at, size)

    def first_coefs(side, where):
        a, b = ranges(side, 0, soon)
        c, d = ranges(side, soon, soon)
        i = 3 * side
        j = 3 * (1 - side)
        return [
            remote(src.at[0, c], src.at[0, d], s_c.at[i], r_c.at[j], where),
            remote(src.at[:, a], src.at[:, b], s_c.at[i + 1], r_c.at[j + 1], where),
            remote(vel.at[a], vel.at[b], s_c.at[i + 2], r_c.at[j + 2], where),
        ]

    def later_coefs(side, where):
        a, b = ranges(side, soon, halo - soon)
        c, _ = ranges(side, 2 * soon, soon)
        d, _ = ranges(side, soon, rest)
        i = 6 + 3 * side
        j = 6 + 3 * (1 - side)
        return [
            remote(src.at[0, c], far.at[1 - side, 0, pl.ds(0, soon)], s_c.at[i], r_c.at[j], where),
            remote(src.at[pl.ds(1, nck - 1), d], far.at[1 - side, pl.ds(1, nck - 1)], s_c.at[i + 1], r_c.at[j + 1], where),
            remote(vel.at[a], vel.at[b], s_c.at[i + 2], r_c.at[j + 2], where),
        ]

    def newer_copies(e, newer):
        def make(side, where):
            a, b = ranges(side, 0, nz)
            return [remote(newer.at[a], newer.at[b], s_f.at[e, side, 0], r_f.at[e, 1 - side, 0], where)]
        return pairs(make)

    def older_copies(e, older):
        def make(side, where):
            a, b = ranges(side, 2, halo - 4)
            return [remote(older.at[a], older.at[b], s_f.at[e, side, 1], r_f.at[e, 1 - side, 1], where)]
        return pairs(make)

    def launch(copies):
        to_lo, to_hi = copies

        @pl.when(has_hi)
        def _():
            for c in to_hi:
                c.start()

        @pl.when(has_lo)
        def _():
            for c in to_lo:
                c.start()

    def settle(copies):
        to_lo, to_hi = copies

        @pl.when(has_hi)
        def _():
            for c in to_lo:
                c.wait_recv()
            for c in to_hi:
                c.wait_send()

        @pl.when(has_lo)
        def _():
            for c in to_hi:
                c.wait_recv()
            for c in to_lo:
                c.wait_send()

    opening, closing = pairs(first_coefs), pairs(later_coefs)
    launch(opening)
    launch(closing)

    def sent_in(c, carry):
        @pl.when(gz * per + c != pos)
        def _():
            remote(stage.at[c], arrival(my_row), s_in.at[c], r_in.at[my_row], lo_id).wait_send()

        return carry

    lax.fori_loop(0, per, sent_in, 0)
    settle(opening)

    def spread(ref, at, size):
        f = ref[pl.ds(at, size)]
        near, wide = plane.lateral(f)
        near = near + (ref[pl.ds(at + 1, size)] + ref[pl.ds(at - 1, size)])
        wide = wide + (ref[pl.ds(at + 2, size)] + ref[pl.ds(at - 2, size)])
        return wide - 16.0 * near + 90.0 * f, f

    def groups(width):
        lo, hi = nz - width, 2 * nz + width
        for at in range(lo, hi, GROUP):
            yield at, min(GROUP, hi - at)

    def forward_step(t, width):
        k = ck_in[t]
        for at, size in groups(width):
            here = pl.ds(at, size)
            lap, f = spread(hist.at[t - 1], at, size)
            value = 2.0 * f + vel[here] * lap + src[k, here]
            if t > 1:
                value = value - hist[t - 2, here]
            hist[t, here] = value

    def adjoint_step(t, width):
        k = ck_in[t]
        first = t == steps - 1
        if not first:
            for at, size in groups(width + 2):
                here = pl.ds(at, size)
                wbuf[here] = vel[here] * adj[t + 1, here]
        for at, size in groups(width):
            here = pl.ds(at, size)
            value = count[here] * hist[t, here]
            if not first:
                lap, _ = spread(wbuf, at, size)
                value = value + lap + 2.0 * adj[t + 1, here]
                if t < steps - 2:
                    value = value - adj[t + 2, here]
            adj[t, here] = value
        img[...] = img[...] + adj[t, nz : 2 * nz] * own_bg[k]

    blocks = steps // BLOCK

    for z in range(nz - 2 * soon, 2 * nz + 2 * soon):
        for c in range(2):
            hist[0, z, c] = src[0, z, c]
    forward_step(1, 2)
    older = older_copies(0, hist.at[1])
    launch(older)
    forward_step(2, 0)
    newer = newer_copies(0, hist.at[2])
    launch(newer)
    settle(closing)

    @pl.when(has_lo)
    def _():
        src[0, nz - halo + 2 : nz - halo + 2 + soon] = far[0, 0, 0:soon]
        src[1:, nz - halo + 2 : nz - soon] = far[0, 1:]

    @pl.when(has_hi)
    def _():
        src[0, 2 * nz + 2 * soon : 2 * nz + 3 * soon] = far[1, 0, 0:soon]
        src[1:, 2 * nz + soon : 2 * nz + 3 * soon] = far[1, 1:]

    settle(older)
    settle(newer)

    def forward_block(b):
        t = b * BLOCK - 1
        for j in range(BLOCK - 1):
            forward_step(t + j, halo - 2 * (j + 1))
        older = older_copies(b, hist.at[t + BLOCK - 2])
        launch(older)
        forward_step(t + BLOCK - 1, 0)
        newer = newer_copies(b, hist.at[t + BLOCK - 1])
        launch(newer)
        settle(older)
        settle(newer)

    for b in range(1, blocks):
        forward_block(b)

    def send_back(src_ref, dst, ss, rs, slot, g):
        def one(row, carry):
            other = (row != my_row) | (g != gz)
            piece = src_ref.at[pl.ds(pl.multiple_of(row * nz, nz), nz)]

            @pl.when(other)
            def _():
                remote(piece, dst.at[slot], ss.at[row], rs.at[slot], (row // gys, row % gys, g)).start()

            @pl.when(jnp.logical_not(other))
            def _():
                dst[slot] = piece[...]

            return carry

        lax.fori_loop(0, rows, one, 0)

    def sent_back(src_ref, dst, ss, rs, g):
        def one(row, carry):
            @pl.when((row != my_row) | (g != gz))
            def _():
                remote(src_ref.at[pl.ds(0, nz)], dst.at[0], ss.at[row], rs.at[0], lo_id).wait_send()

            return carry

        lax.fori_loop(0, rows, one, 0)

    def got_back(src_ref, dst, ss, rs, first, number):
        def one(c, carry):
            @pl.when(c + first != pos)
            def _():
                remote(src_ref.at[pl.ds(0, nz)], dst.at[c], ss.at[0], rs.at[c], lo_id).wait_recv()

            return carry

        lax.fori_loop(0, number, one, 0)

    near = 4
    apart = n // near
    team, seat = pos // near, pos % near

    def trace_sends(src_ref, dst, kind):
        number = near if kind == 0 else apart
        mine = seat if kind == 0 else team

        def one(i, carry):
            @pl.when(i != mine)
            def _():
                p = team * near + i if kind == 0 else i * near + seat
                remote(src_ref, dst.at[mine], s_t.at[kind, i], r_t.at[kind, mine], place_of(p, gxs, gys, gzs)).start()

            return carry

        lax.fori_loop(0, number, one, 0)

    def trace_waits(src_ref, dst, kind):
        number = near if kind == 0 else apart
        mine = seat if kind == 0 else team

        def one(i, carry):
            @pl.when(i != mine)
            def _():
                remote(src_ref, dst.at[i], s_t.at[kind, i], r_t.at[kind, i], lo_id).wait()

            return carry

        lax.fori_loop(0, number, one, 0)

    def gather_traces():
        picked = one_zr[nz * rows : 2 * nz * rows]
        lane_pick = one_lane.astype(jnp.bfloat16)
        lines = []
        for t in range(steps):
            table = hist[t, nz : 2 * nz].reshape(nz * rows, lanes)
            at_row = jnp.zeros((nz * rows, nrec), f32)
            for _ in range(3):
                piece = table.astype(jnp.bfloat16)
                at_row = at_row + jnp.dot(piece, lane_pick, preferred_element_type=f32)
                table = table - piece.astype(f32)
            lines.append(jnp.sum(at_row * picked, axis=0, keepdims=True))
        return jnp.concatenate(lines, axis=0)

    def give_back(read, dst):
        for z in range(nz):
            for g, value in enumerate(plane.split(*read(z))):
                dst[pl.ds(g * nz + z, gxs, stride=gys * nz), :] = value

    last = steps - 1
    forward_step(last, halo - 2)
    adjoint_step(last, halo - 2)
    adjoint_step(last - 1, halo - 4)
    adjoint_step(last - 2, halo - 6)
    older = older_copies(blocks, adj.at[last - 2])
    launch(older)
    adjoint_step(last - 3, 0)
    newer = newer_copies(blocks, adj.at[last - 3])
    launch(newer)
    give_back(lambda z: (hist[last, nz + z, 0], hist[last, nz + z, 1]), back_w)
    send_back(back_w, in_w, s_w, r_w, lax.rem(pos, per), owner)
    part[0] = gather_traces()
    tr1[seat] = part[0]
    trace_sends(part.at[0], tr1, 0)
    settle(older)
    settle(newer)

    def trace_relay():
        trace_waits(part.at[0], tr1, 0)
        total = tr1[0]
        for i in range(1, near):
            total = total + tr1[i]
        part[1] = total
        tr2[team] = total
        trace_sends(part.at[1], tr2, 1)

    def adjoint_block(b):
        t = last - BLOCK * b
        for j in range(BLOCK - 1):
            adjoint_step(t - j, halo - 2 * (j + 1))
        if b == blocks - 1:
            adjoint_step(t - BLOCK + 1, 0)
            return
        older = older_copies(blocks + b, adj.at[t - BLOCK + 2])
        launch(older)
        adjoint_step(t - BLOCK + 1, 0)
        newer = newer_copies(blocks + b, adj.at[t - BLOCK + 1])
        launch(newer)
        if b == 1:
            trace_relay()
        settle(older)
        settle(newer)

    for b in range(1, blocks):
        adjoint_block(b)

    give_back(lambda z: (img[z, 0], img[z, 1]), back_i)
    send_back(back_i, in_i, s_i, r_i, lax.rem(pos, per), owner)
    sums = [img[0, c] for c in range(2)]
    for z in range(1, nz):
        sums = [sums[c] + img[z, c] for c in range(2)]
    for g, value in enumerate(plane.split(*sums)):
        for i in range(gxs):
            back_c[i * gys + g] = value[i : i + 1]

    def send_sums(i, carry):
        row, g = i // gzs, i % gzs
        other = (row != my_row) | (g != gz)

        @pl.when(other)
        def _():
            remote(back_c.at[row], in_c.at[pos], s_k.at[i], r_k.at[pos], (row // gys, row % gys, g)).start()

        @pl.when(jnp.logical_not(other))
        def _():
            in_c[pos] = back_c[row]

        return carry

    lax.fori_loop(0, n, send_sums, 0)

    trace_waits(part.at[1], tr2, 1)
    total = tr2[0]
    for i in range(1, apart):
        total = total + tr2[i]
    traces_ref[...] = total

    def put_out(buffer, out_ref):
        turned = buffer[...].reshape(sz, lanes).T
        for k in range(sx):
            out_ref[quarter_owner(k, gy)] = turned[k * sy : (k + 1) * sy]

    got_back(back_w, in_w, s_w, r_w, gz * per, per)
    put_out(in_w, wave_ref)
    sent_back(back_w, in_w, s_w, r_w, owner)

    got_back(back_i, in_i, s_i, r_i, gz * per, per)
    put_out(in_i, image_ref)

    def got_sums(i, carry):
        @pl.when(i != pos)
        def _():
            remote(back_c.at[0], in_c.at[i], s_k.at[0], r_k.at[i], lo_id).wait_recv()

        return carry

    lax.fori_loop(0, n, got_sums, 0)
    depth = in_c[0]
    for i in range(1, n):
        depth = depth + in_c[i]
    depth = depth / (sz * gzs)
    for k in range(sx):
        column_ref[pl.ds(quarter_owner(k, gy), 1), :] = depth[:, k * sy : (k + 1) * sy]
    sent_back(back_i, in_i, s_i, r_i, owner)

    def sent_sums(i, carry):
        @pl.when((i // gzs != my_row) | (i % gzs != gz))
        def _():
            remote(back_c.at[0], in_c.at[0], s_k.at[i], r_k.at[0], lo_id).wait_send()

        return carry

    lax.fori_loop(0, n, sent_sums, 0)


def store_kernel(*refs):
    count = len(refs) // 2
    ins, outs, sems = refs[:count], refs[count : 2 * count], refs[2 * count]
    copies = [pltpu.make_async_copy(a, b, sems.at[i]) for i, (a, b) in enumerate(zip(ins, outs))]
    for copy in copies:
        copy.start()
    for copy in copies:
        copy.wait()


def chain_on_device(sizes, velocity_term, model_step, background, receivers, checkpoints):
    gxs, gys, gzs = sizes
    sx, sy, sz = model_step.shape
    nck, steps, nrec = background.shape[0], checkpoints.shape[0], receivers.shape[1]
    n, rows, lanes = gxs * gys * gzs, gxs * gys, sx * sy
    nz = sz * gzs // n
    per = sz // nz
    ext = 3 * nz
    blocks = steps // BLOCK
    halo = 2 * BLOCK
    dims = (gxs, gys, gzs, sx, sy, sz, nck, steps)
    f32 = jnp.float32
    dma = pltpu.SemaphoreType.DMA
    vmem = pl.BlockSpec(memory_space=pltpu.VMEM)
    hbm = pl.BlockSpec(memory_space=pltpu.HBM)
    tile = (2, gxs, lanes)
    shapes = (
        jax.ShapeDtypeStruct((sx, sy, sz), f32),
        jax.ShapeDtypeStruct((steps, nrec), f32),
        jax.ShapeDtypeStruct((sx, sy), f32),
        jax.ShapeDtypeStruct((sx, sy, sz), f32),
    )
    results = pl.pallas_call(
        functools.partial(chain_kernel, dims),
        out_shape=shapes,
        in_specs=[hbm] * 5,
        out_specs=(vmem,) * 4,
        scratch_shapes=[
            pltpu.VMEM(velocity_term.shape, f32),
            pltpu.VMEM(model_step.shape, f32),
            pltpu.VMEM(background.shape, background.dtype),
            pltpu.VMEM(receivers.shape, receivers.dtype),
            pltpu.SMEM(checkpoints.shape, checkpoints.dtype),
            pltpu.VMEM((per, (2 + nck) * nz, lanes), f32),
            pltpu.VMEM((rows * (2 + nck) * nz, lanes), f32),
            pltpu.VMEM((ext,) + tile, f32),
            pltpu.VMEM((nck, ext) + tile, f32),
            pltpu.VMEM((2, nck, halo // 2) + tile, f32),
            pltpu.VMEM((nck, nz) + tile, f32),
            pltpu.VMEM((steps, ext) + tile, f32),
            pltpu.VMEM((steps, ext) + tile, f32),
            pltpu.VMEM((ext,) + tile, f32),
            pltpu.VMEM((nz,) + tile, f32),
            pltpu.VMEM((ext,) + tile, f32),
            pltpu.VMEM((2, steps, nrec), f32),
            pltpu.VMEM((4, steps, nrec), f32),
            pltpu.VMEM((n // 4, steps, nrec), f32),
            pltpu.VMEM((rows * nz, lanes), f32),
            pltpu.VMEM((rows * nz, lanes), f32),
            pltpu.VMEM((rows, 1, lanes), f32),
            pltpu.VMEM((per, nz, lanes), f32),
            pltpu.VMEM((per, nz, lanes), f32),
            pltpu.VMEM((n, 1, lanes), f32),
            dma((5,)),
            dma((per,)),
            dma((rows,)),
            dma((12,)),
            dma((12,)),
            dma((2 * blocks - 1, 2, 2)),
            dma((2 * blocks - 1, 2, 2)),
            dma((2, max(4, n // 4))),
            dma((2, max(4, n // 4))),
            dma((rows,)),
            dma((per,)),
            dma((rows,)),
            dma((per,)),
            dma((n,)),
            dma((n,)),
        ],
        compiler_params=pltpu.CompilerParams(
            collective_id=0, has_side_effects=True, vmem_limit_bytes=48 * 1024 * 1024
        ),
    )(velocity_term, model_step, background, receivers, checkpoints)
    return pl.pallas_call(
        store_kernel,
        out_shape=shapes,
        in_specs=[vmem] * 4,
        out_specs=(hbm,) * 4,
        scratch_shapes=[dma((4,))],
    )(*results)


def solution(mesh):
    gxs, gys, gzs = mesh.shape["gx"], mesh.shape["gy"], mesh.shape["gz"]
    n = gxs * gys * gzs

    def whole(velocity_term, model_step, background, receivers, checkpoints):
        nx, ny, depth = model_step.shape
        fits = (
            depth % (8 * n) == 0
            and depth // n == 2 * BLOCK
            and gxs == 8
            and gys == 2
            and n % 4 == 0
            and nx // gxs == 4
            and (nx // gxs) * (ny // gys) == 128
            and checkpoints.shape[0] == 4 * BLOCK
        )
        body = functools.partial(chain_on_device, (gxs, gys, gzs)) if fits else on_device
        return jax.shard_map(
            body,
            mesh=mesh,
            in_specs=(P("gx", "gy", "gz"), P("gx", "gy", "gz"), P(None, "gx", "gy", "gz"), P(), P()),
            out_specs=(P("gx", "gy", "gz"), P(), P("gx", "gy"), P("gx", "gy", "gz")),
            check_vma=False,
        )(velocity_term, model_step, background, receivers, checkpoints)

    return whole
```

```python
import functools

import jax
import jax.numpy as jnp
from jax import lax
from jax.experimental import pallas as pl
from jax.experimental.pallas import tpu as pltpu
from jax.sharding import PartitionSpec as P

near_coef = 4.0 / 3.0
far_coef = -1.0 / 12.0
center_coef = -2.5


def with_halo(block, sides, width, periodic):
    for axis, dim in sides:
        count = lax.axis_size(axis)
        forward = [(i, i + 1) for i in range(count - 1)]
        if periodic:
            forward.append((count - 1, 0))
        backward = [(target, source) for source, target in forward]
        low = lax.ppermute(
            lax.slice_in_dim(block, block.shape[dim] - width, None, axis=dim), axis, forward
        )
        high = lax.ppermute(lax.slice_in_dim(block, 0, width, axis=dim), axis, backward)
        block = jnp.concatenate([low, block, high], axis=dim)
    return block


def along(padded, dim):
    count = padded.shape[dim]
    first = lax.slice_in_dim(padded, 3, count - 1, axis=dim) + lax.slice_in_dim(
        padded, 1, count - 3, axis=dim
    )
    second = lax.slice_in_dim(padded, 4, count, axis=dim) + lax.slice_in_dim(
        padded, 0, count - 4, axis=dim
    )
    return near_coef * first + far_coef * second


def laplace(field):
    side = with_halo(field, (("gx", 0), ("gy", 1)), 2, True)
    deep = with_halo(field, (("gz", 2),), 2, False)
    x_pad = side[:, 2:-2, :]
    y_pad = side[2:-2, :, :]
    return 3.0 * center_coef * field + along(x_pad, 0) + along(y_pad, 1) + along(deep, 2)


def sample_row(samples, field, step, clip_x, clip_y, clip_z, inside):
    values = field[clip_x, clip_y, clip_z] * inside
    return lax.dynamic_update_index_in_dim(samples, values, step, 0)


def on_device(velocity_term, model_step, background, receivers, checkpoints):
    size_x, size_y, size_z = model_step.shape
    steps = checkpoints.shape[0]
    local_x = receivers[0] - lax.axis_index("gx") * size_x
    local_y = receivers[1] - lax.axis_index("gy") * size_y
    local_z = receivers[2] - lax.axis_index("gz") * size_z
    inside = (
        (local_x >= 0)
        & (local_x < size_x)
        & (local_y >= 0)
        & (local_y < size_y)
        & (local_z >= 0)
        & (local_z < size_z)
    )
    inside = inside.astype(jnp.float32)
    clip_x = jnp.clip(local_x, 0, size_x - 1)
    clip_y = jnp.clip(local_y, 0, size_y - 1)
    clip_z = jnp.clip(local_z, 0, size_z - 1)
    zeros = jnp.zeros(model_step.shape, jnp.float32)
    record = jnp.zeros((steps, receivers.shape[1]), jnp.float32)

    def forward(step, carry):
        previous, current, samples = carry
        accel = lax.dynamic_index_in_dim(background, checkpoints[step], 0, keepdims=False).astype(
            jnp.float32
        )
        following = 2.0 * current - previous + velocity_term * laplace(current) + model_step * accel
        samples = sample_row(samples, following, step, clip_x, clip_y, clip_z, inside)
        return (current, following, samples)

    previous, current, record = lax.fori_loop(0, steps, forward, (zeros, zeros, record))
    traces = lax.psum(record, ("gx", "gy", "gz"))

    def adjoint_step(back, carry):
        later_two, later, image = carry
        step = steps - 1 - back
        accel = lax.dynamic_index_in_dim(background, checkpoints[step], 0, keepdims=False).astype(
            jnp.float32
        )
        adjoint = 2.0 * later - later_two + laplace(velocity_term * later)
        inject = lax.dynamic_index_in_dim(traces, step, 0, keepdims=False) * inside
        adjoint = adjoint.at[clip_x, clip_y, clip_z].add(inject)
        return (later, adjoint, image + adjoint * accel)

    later_two, later, image = lax.fori_loop(0, steps, adjoint_step, (zeros, zeros, zeros))
    depth_total = size_z * lax.axis_size("gz")
    column_image = lax.psum(jnp.sum(image, axis=2), "gz") / depth_total
    return (image, traces, column_image, current)


MESH = pl.DeviceIdType.MESH
BLOCK = 4
GROUP = 4


def place_of(p, gxs, gys, gzs):
    q, gz = p // gzs, p % gzs
    per = 2 * gys
    zz, w = q // per, q % per
    w = w + (zz % 2) * (per - 1 - 2 * w)
    xx, yy = w // gys, w % gys
    return 2 * zz + xx, yy + xx * (gys - 1 - 2 * yy), gz


def position_of(gx, gy, gz, gxs, gys, gzs):
    per = 2 * gys
    zz, xx = gx // 2, gx % 2
    w = xx * gys + gy + xx * (gys - 1 - 2 * gy)
    w = w + (zz % 2) * (per - 1 - 2 * w)
    return (zz * per + w) * gzs + gz


def lane_roll(a, k):
    return pltpu.roll(a, k % a.shape[-1], a.ndim - 1)


def row_roll(a, k):
    return pltpu.roll(a, k % a.shape[-2], a.ndim - 2)


def quarter_owner(k, gy):
    base = (k % 2) * 2 + k // 2
    return base + gy * (2 - 4 * (k % 2))


class Plane:
    def __init__(self, rows, lanes):
        half = lanes // 2
        lane = lax.broadcasted_iota(jnp.int32, (rows, lanes), 1)
        self.half = half
        self.even = lane < half
        self.odd_quarter = lane % half >= half // 2

    def swap_quarters(self, a):
        quarter = self.half // 2
        return jnp.where(self.odd_quarter, lane_roll(a, quarter), lane_roll(a, -quarter))

    def join(self, low, high):
        return (
            jnp.where(self.odd_quarter, high, low),
            self.swap_quarters(jnp.where(self.odd_quarter, low, high)),
        )

    def split(self, f0, f1):
        t = self.swap_quarters(f1)
        return jnp.where(self.odd_quarter, t, f0), jnp.where(self.odd_quarter, f0, t)

    def taps(self):
        lanes = 2 * self.half
        shape = (2 * lanes, 2 * lanes)
        i, j = lax.broadcasted_iota(jnp.int32, shape, 0) % lanes, lax.broadcasted_iota(jnp.int32, shape, 1)
        across = (i - j + lanes) % lanes == self.half
        shift = (j - i + lanes) % self.half
        same = (i < self.half) == (j < self.half)
        near = same & ((shift == 1) | (shift == self.half - 1))
        far = same & ((shift == 2) | (shift == self.half - 2))
        beside = jnp.where(near, -16.0, 0.0) + jnp.where(far, 1.0, 0.0)
        return (jnp.where(j < lanes, beside, 0.0) + jnp.where(across, -16.0, 0.0)).astype(jnp.bfloat16)

    def lateral(self, f, y_sum, other):
        x0, x1, f0, f1 = other[:, 0], other[:, 1], f[:, 0], f[:, 1]
        low = jnp.where(self.even, row_roll(x1, 1), x1) + (f1 + row_roll(f1, 1))
        high = jnp.where(self.even, x0, row_roll(x0, -1)) + (f0 + row_roll(f0, -1))
        return y_sum + jnp.stack([low, high], axis=1)


def chain_kernel(
    dims, v_hbm, m_hbm, bg_hbm, rec_hbm, ck_hbm,
    image_ref, traces_ref, column_ref, wave_ref,
    v_in, m_in, bg_in, rec_in, ck_in,
    stage, landed, vel, src, far, own_bg, hist, adj, wbuf, taps, mixed, img, count, part, tr1, tr2,
    back_w, back_i, back_c, in_w, in_i, in_c,
    s_0, s_in, r_in, s_c, r_c, s_f, r_f, s_t, r_t, s_w, r_w, s_i, r_i, s_k, r_k,
):
    gxs, gys, gzs, sx, sy, sz, nck, steps = dims
    n = gxs * gys * gzs
    rows = gxs * gys
    lanes = sx * sy
    nz = sz * gzs // n
    per = sz // nz
    fields = 2 + nck
    gx, gy, gz = lax.axis_index("gx"), lax.axis_index("gy"), lax.axis_index("gz")
    pos = position_of(gx, gy, gz, gxs, gys, gzs)
    my_row = gx * gys + gy
    lo_id = place_of(jnp.maximum(pos - 1, 0), gxs, gys, gzs)
    hi_id = place_of(jnp.minimum(pos + 1, n - 1), gxs, gys, gzs)
    has_lo, has_hi = pos > 0, pos < n - 1
    ext = 3 * nz
    f32 = jnp.float32
    tile = (gxs, lanes)

    def remote(src_ref, dst_ref, ss, rs, where):
        return pltpu.make_async_remote_copy(
            src_ref=src_ref, dst_ref=dst_ref, send_sem=ss, recv_sem=rs, device_id=where, device_id_type=MESH
        )

    barrier = pltpu.get_barrier_semaphore()

    def greet(p, carry):
        @pl.when(p != pos)
        def _():
            pl.semaphore_signal(barrier, inc=1, device_id=place_of(p, gxs, gys, gzs), device_id_type=MESH)
        return carry

    loads = [
        pltpu.make_async_copy(a, b, s_0.at[i])
        for i, (a, b) in enumerate(
            ((v_hbm, v_in), (m_hbm, m_in), (bg_hbm, bg_in), (rec_hbm, rec_in), (ck_hbm, ck_in))
        )
    ]
    for load in loads:
        load.start()
    lax.fori_loop(0, n, greet, 0)

    plane = Plane(gxs, lanes)

    @pl.when(jnp.logical_not(has_lo))
    def _():
        vel[0:nz] = jnp.zeros((nz, 2) + tile, f32)
        for k in range(nck):
            src[k, 0:nz] = jnp.zeros((nz, 2) + tile, f32)
        for t in range(steps):
            hist[t, 0:nz] = jnp.zeros((nz, 2) + tile, f32)
            adj[t, 0:nz] = jnp.zeros((nz, 2) + tile, f32)

    @pl.when(jnp.logical_not(has_hi))
    def _():
        vel[2 * nz :] = jnp.zeros((nz, 2) + tile, f32)
        for k in range(nck):
            src[k, 2 * nz :] = jnp.zeros((nz, 2) + tile, f32)
        for t in range(steps):
            hist[t, 2 * nz :] = jnp.zeros((nz, 2) + tile, f32)
            adj[t, 2 * nz :] = jnp.zeros((nz, 2) + tile, f32)

    for load in loads[:3]:
        load.wait()
    for f in range(fields):
        pieces = []
        for k in range(sx):
            x = quarter_owner(k, gy)
            if f == 0:
                pieces.append(v_in[x])
            elif f == 1:
                pieces.append(m_in[x])
            else:
                pieces.append(bg_in[f - 2, x].astype(f32))
        turned = jnp.concatenate(pieces, axis=0).T
        stage[:, f * nz : (f + 1) * nz, :] = turned.reshape(per, nz, lanes)
    pl.semaphore_wait(barrier, n - 1)

    slab = fields * nz

    def arrival(row):
        return landed.at[pl.ds(pl.multiple_of(row * slab, nz), slab)]

    def scatter_in(c, carry):
        p = gz * per + c

        @pl.when(p != pos)
        def _():
            remote(stage.at[c], arrival(my_row), s_in.at[c], r_in.at[my_row], place_of(p, gxs, gys, gzs)).start()

        @pl.when(p == pos)
        def _():
            landed[pl.ds(pl.multiple_of(my_row * slab, nz), slab), :] = stage[c]

        return carry

    lax.fori_loop(0, per, scatter_in, 0)

    for load in loads[3:]:
        load.wait()
    rec = rec_in[...]
    rx, ry, rz = rec[0:1], rec[1:2], rec[2:3]
    nrec = rec.shape[1]
    rlane = (rx % 2) * (lanes // 2) + ry
    rlocal = rz - (pos - 1) * nz
    zr = jnp.where((rlocal >= 0) & (rlocal < ext), (rlocal * 2 + (rx % sx) // 2) * gxs + rx // sx, -1)
    one_zr = (lax.broadcasted_iota(jnp.int32, (ext * rows, nrec), 0) == zr).astype(f32)
    one_lane = (lax.broadcasted_iota(jnp.int32, (lanes, nrec), 0) == rlane).astype(f32)
    counted = lax.dot_general(
        one_zr.astype(jnp.bfloat16), one_lane.astype(jnp.bfloat16), (((1,), (1,)), ((), ())),
        preferred_element_type=f32,
    )
    count[...] = counted.reshape((ext, 2) + tile)
    img[...] = jnp.zeros_like(img)
    taps[...] = plane.taps()

    owner = pos // per

    def wait_in(row, carry):
        sender = row // gys, row % gys, owner

        @pl.when((row != my_row) | (owner != gz))
        def _():
            remote(stage.at[0], arrival(row), s_in.at[0], r_in.at[row], sender).wait_recv()

        return carry

    lax.fori_loop(0, rows, wait_in, 0)

    def gathered(f, z):
        low = landed[pl.ds(f * nz + z, gxs, stride=gys * slab), :]
        high = landed[pl.ds(slab + f * nz + z, gxs, stride=gys * slab), :]
        return plane.join(low, high)

    for z in range(nz):
        vs = gathered(0, z)
        ms = gathered(1, z)
        for c in range(2):
            vel[nz + z, c] = far_coef * vs[c]
        for k in range(nck):
            accel = gathered(2 + k, z)
            for c in range(2):
                own_bg[k, z, c] = accel[c]
                src[k, nz + z, c] = ms[c] * accel[c]

    halo = 2 * BLOCK
    soon, rest = halo // 4, halo // 2

    def pairs(make):
        return make(0, lo_id), make(1, hi_id)

    def ranges(side, near_at, size):
        at = nz - near_at - size if side else near_at
        return pl.ds(nz + at, size), pl.ds(at if side else 2 * nz + at, size)

    def first_coefs(side, where):
        a, b = ranges(side, 0, soon)
        c, d = ranges(side, soon, soon)
        i = 3 * side
        j = 3 * (1 - side)
        return [
            remote(src.at[0, c], src.at[0, d], s_c.at[i], r_c.at[j], where),
            remote(src.at[:, a], src.at[:, b], s_c.at[i + 1], r_c.at[j + 1], where),
            remote(vel.at[a], vel.at[b], s_c.at[i + 2], r_c.at[j + 2], where),
        ]

    def later_coefs(side, where):
        a, b = ranges(side, soon, halo - soon)
        c, _ = ranges(side, 2 * soon, soon)
        d, _ = ranges(side, soon, rest)
        i = 6 + 3 * side
        j = 6 + 3 * (1 - side)
        return [
            remote(src.at[0, c], far.at[1 - side, 0, pl.ds(0, soon)], s_c.at[i], r_c.at[j], where),
            remote(src.at[pl.ds(1, nck - 1), d], far.at[1 - side, pl.ds(1, nck - 1)], s_c.at[i + 1], r_c.at[j + 1], where),
            remote(vel.at[a], vel.at[b], s_c.at[i + 2], r_c.at[j + 2], where),
        ]

    def newer_copies(e, newer):
        def make(side, where):
            a, b = ranges(side, 0, nz)
            return [remote(newer.at[a], newer.at[b], s_f.at[e, side, 0], r_f.at[e, 1 - side, 0], where)]
        return pairs(make)

    def older_copies(e, older):
        def make(side, where):
            a, b = ranges(side, 2, halo - 4)
            return [remote(older.at[a], older.at[b], s_f.at[e, side, 1], r_f.at[e, 1 - side, 1], where)]
        return pairs(make)

    def launch(copies):
        to_lo, to_hi = copies

        @pl.when(has_hi)
        def _():
            for c in to_hi:
                c.start()

        @pl.when(has_lo)
        def _():
            for c in to_lo:
                c.start()

    def settle(copies):
        to_lo, to_hi = copies

        @pl.when(has_hi)
        def _():
            for c in to_lo:
                c.wait_recv()
            for c in to_hi:
                c.wait_send()

        @pl.when(has_lo)
        def _():
            for c in to_hi:
                c.wait_recv()
            for c in to_lo:
                c.wait_send()

    opening, closing = pairs(first_coefs), pairs(later_coefs)
    launch(opening)
    launch(closing)

    def sent_in(c, carry):
        @pl.when(gz * per + c != pos)
        def _():
            remote(stage.at[c], arrival(my_row), s_in.at[c], r_in.at[my_row], lo_id).wait_send()

        return carry

    lax.fori_loop(0, per, sent_in, 0)
    settle(opening)

    def lateral_sums(ref, width):
        size = nz + 2 * width
        f = ref[pl.ds(nz - width, size)].reshape(size * rows, lanes)
        top = f.astype(jnp.bfloat16)
        low = (f - top.astype(f32)).astype(jnp.bfloat16)
        mixed[pl.ds((nz - width) * rows, size * rows)] = jnp.dot(
            jnp.concatenate([top, low], axis=1), taps[...], preferred_element_type=f32
        )

    def spread(ref, at, size):
        f = ref[pl.ds(at, size)]
        m = pl.ds(at * rows, size * rows)
        shape = (size, 2) + tile
        near = ref[pl.ds(at + 1, size)] + ref[pl.ds(at - 1, size)]
        wide = ref[pl.ds(at + 2, size)] + ref[pl.ds(at - 2, size)]
        flat = plane.lateral(f, mixed[m, 0:lanes].reshape(shape), mixed[m, lanes : 2 * lanes].reshape(shape))
        return flat + wide - 16.0 * near + 90.0 * f, f

    def groups(width):
        lo, hi = nz - width, 2 * nz + width
        for at in range(lo, hi, GROUP):
            yield at, min(GROUP, hi - at)

    def forward_step(t, width):
        k = ck_in[t]
        lateral_sums(hist.at[t - 1], width)
        for at, size in groups(width):
            here = pl.ds(at, size)
            lap, f = spread(hist.at[t - 1], at, size)
            value = 2.0 * f + vel[here] * lap + src[k, here]
            if t > 1:
                value = value - hist[t - 2, here]
            hist[t, here] = value

    def adjoint_step(t, width):
        k = ck_in[t]
        first = t == steps - 1
        if not first:
            for at, size in groups(width + 2):
                here = pl.ds(at, size)
                wbuf[here] = vel[here] * adj[t + 1, here]
            lateral_sums(wbuf, width)
        for at, size in groups(width):
            here = pl.ds(at, size)
            value = count[here] * hist[t, here]
            if not first:
                lap, _ = spread(wbuf, at, size)
                value = value + lap + 2.0 * adj[t + 1, here]
                if t < steps - 2:
                    value = value - adj[t + 2, here]
            adj[t, here] = value
        img[...] = img[...] + adj[t, nz : 2 * nz] * own_bg[k]

    blocks = steps // BLOCK

    for z in range(nz - 2 * soon, 2 * nz + 2 * soon):
        for c in range(2):
            hist[0, z, c] = src[0, z, c]
    forward_step(1, 2)
    older = older_copies(0, hist.at[1])
    launch(older)
    forward_step(2, 0)
    newer = newer_copies(0, hist.at[2])
    launch(newer)
    settle(closing)

    @pl.when(has_lo)
    def _():
        src[0, nz - halo + 2 : nz - halo + 2 + soon] = far[0, 0, 0:soon]
        src[1:, nz - halo + 2 : nz - soon] = far[0, 1:]

    @pl.when(has_hi)
    def _():
        src[0, 2 * nz + 2 * soon : 2 * nz + 3 * soon] = far[1, 0, 0:soon]
        src[1:, 2 * nz + soon : 2 * nz + 3 * soon] = far[1, 1:]

    settle(older)
    settle(newer)

    def forward_block(b):
        t = b * BLOCK - 1
        for j in range(BLOCK - 1):
            forward_step(t + j, halo - 2 * (j + 1))
        older = older_copies(b, hist.at[t + BLOCK - 2])
        launch(older)
        forward_step(t + BLOCK - 1, 0)
        newer = newer_copies(b, hist.at[t + BLOCK - 1])
        launch(newer)
        settle(older)
        settle(newer)

    for b in range(1, blocks):
        forward_block(b)

    def send_back(src_ref, dst, ss, rs, slot, g):
        def one(row, carry):
            other = (row != my_row) | (g != gz)
            piece = src_ref.at[pl.ds(pl.multiple_of(row * nz, nz), nz)]

            @pl.when(other)
            def _():
                remote(piece, dst.at[slot], ss.at[row], rs.at[slot], (row // gys, row % gys, g)).start()

            @pl.when(jnp.logical_not(other))
            def _():
                dst[slot] = piece[...]

            return carry

        lax.fori_loop(0, rows, one, 0)

    def sent_back(src_ref, dst, ss, rs, g):
        def one(row, carry):
            @pl.when((row != my_row) | (g != gz))
            def _():
                remote(src_ref.at[pl.ds(0, nz)], dst.at[0], ss.at[row], rs.at[0], lo_id).wait_send()

            return carry

        lax.fori_loop(0, rows, one, 0)

    def got_back(src_ref, dst, ss, rs, first, number):
        def one(c, carry):
            @pl.when(c + first != pos)
            def _():
                remote(src_ref.at[pl.ds(0, nz)], dst.at[c], ss.at[0], rs.at[c], lo_id).wait_recv()

            return carry

        lax.fori_loop(0, number, one, 0)

    near = 4
    apart = n // near
    team, seat = pos // near, pos % near

    def trace_sends(src_ref, dst, kind):
        number = near if kind == 0 else apart
        mine = seat if kind == 0 else team

        def one(i, carry):
            @pl.when(i != mine)
            def _():
                p = team * near + i if kind == 0 else i * near + seat
                remote(src_ref, dst.at[mine], s_t.at[kind, i], r_t.at[kind, mine], place_of(p, gxs, gys, gzs)).start()

            return carry

        lax.fori_loop(0, number, one, 0)

    def trace_waits(src_ref, dst, kind):
        number = near if kind == 0 else apart
        mine = seat if kind == 0 else team

        def one(i, carry):
            @pl.when(i != mine)
            def _():
                remote(src_ref, dst.at[i], s_t.at[kind, i], r_t.at[kind, i], lo_id).wait()

            return carry

        lax.fori_loop(0, number, one, 0)

    def gather_traces():
        picked = one_zr[nz * rows : 2 * nz * rows]
        lane_pick = one_lane.astype(jnp.bfloat16)
        lines = []
        for t in range(steps):
            table = hist[t, nz : 2 * nz].reshape(nz * rows, lanes)
            at_row = jnp.zeros((nz * rows, nrec), f32)
            for _ in range(3):
                piece = table.astype(jnp.bfloat16)
                at_row = at_row + jnp.dot(piece, lane_pick, preferred_element_type=f32)
                table = table - piece.astype(f32)
            lines.append(jnp.sum(at_row * picked, axis=0, keepdims=True))
        return jnp.concatenate(lines, axis=0)

    def give_back(read, dst):
        for z in range(nz):
            for g, value in enumerate(plane.split(*read(z))):
                dst[pl.ds(g * nz + z, gxs, stride=gys * nz), :] = value

    last = steps - 1
    forward_step(last, halo - 2)
    adjoint_step(last, halo - 2)
    adjoint_step(last - 1, halo - 4)
    adjoint_step(last - 2, halo - 6)
    older = older_copies(blocks, adj.at[last - 2])
    launch(older)
    adjoint_step(last - 3, 0)
    newer = newer_copies(blocks, adj.at[last - 3])
    launch(newer)
    give_back(lambda z: (hist[last, nz + z, 0], hist[last, nz + z, 1]), back_w)
    send_back(back_w, in_w, s_w, r_w, lax.rem(pos, per), owner)
    part[0] = gather_traces()
    tr1[seat] = part[0]
    trace_sends(part.at[0], tr1, 0)
    settle(older)
    settle(newer)

    def trace_relay():
        trace_waits(part.at[0], tr1, 0)
        total = tr1[0]
        for i in range(1, near):
            total = total + tr1[i]
        part[1] = total
        tr2[team] = total
        trace_sends(part.at[1], tr2, 1)

    def adjoint_block(b):
        t = last - BLOCK * b
        for j in range(BLOCK - 1):
            adjoint_step(t - j, halo - 2 * (j + 1))
        if b == blocks - 1:
            adjoint_step(t - BLOCK + 1, 0)
            return
        older = older_copies(blocks + b, adj.at[t - BLOCK + 2])
        launch(older)
        adjoint_step(t - BLOCK + 1, 0)
        newer = newer_copies(blocks + b, adj.at[t - BLOCK + 1])
        launch(newer)
        if b == 1:
            trace_relay()
        settle(older)
        settle(newer)

    for b in range(1, blocks):
        adjoint_block(b)

    give_back(lambda z: (img[z, 0], img[z, 1]), back_i)
    send_back(back_i, in_i, s_i, r_i, lax.rem(pos, per), owner)
    sums = [img[0, c] for c in range(2)]
    for z in range(1, nz):
        sums = [sums[c] + img[z, c] for c in range(2)]
    for g, value in enumerate(plane.split(*sums)):
        for i in range(gxs):
            back_c[i * gys + g] = value[i : i + 1]

    def send_sums(i, carry):
        row, g = i // gzs, i % gzs
        other = (row != my_row) | (g != gz)

        @pl.when(other)
        def _():
            remote(back_c.at[row], in_c.at[pos], s_k.at[i], r_k.at[pos], (row // gys, row % gys, g)).start()

        @pl.when(jnp.logical_not(other))
        def _():
            in_c[pos] = back_c[row]

        return carry

    lax.fori_loop(0, n, send_sums, 0)

    trace_waits(part.at[1], tr2, 1)
    total = tr2[0]
    for i in range(1, apart):
        total = total + tr2[i]
    traces_ref[...] = total

    def put_out(buffer, out_ref):
        turned = buffer[...].reshape(sz, lanes).T
        for k in range(sx):
            out_ref[quarter_owner(k, gy)] = turned[k * sy : (k + 1) * sy]

    got_back(back_w, in_w, s_w, r_w, gz * per, per)
    put_out(in_w, wave_ref)
    sent_back(back_w, in_w, s_w, r_w, owner)

    got_back(back_i, in_i, s_i, r_i, gz * per, per)
    put_out(in_i, image_ref)

    def got_sums(i, carry):
        @pl.when(i != pos)
        def _():
            remote(back_c.at[0], in_c.at[i], s_k.at[0], r_k.at[i], lo_id).wait_recv()

        return carry

    lax.fori_loop(0, n, got_sums, 0)
    depth = in_c[0]
    for i in range(1, n):
        depth = depth + in_c[i]
    depth = depth / (sz * gzs)
    for k in range(sx):
        column_ref[pl.ds(quarter_owner(k, gy), 1), :] = depth[:, k * sy : (k + 1) * sy]
    sent_back(back_i, in_i, s_i, r_i, owner)

    def sent_sums(i, carry):
        @pl.when((i // gzs != my_row) | (i % gzs != gz))
        def _():
            remote(back_c.at[0], in_c.at[0], s_k.at[i], r_k.at[0], lo_id).wait_send()

        return carry

    lax.fori_loop(0, n, sent_sums, 0)


def store_kernel(*refs):
    count = len(refs) // 2
    ins, outs, sems = refs[:count], refs[count : 2 * count], refs[2 * count]
    copies = [pltpu.make_async_copy(a, b, sems.at[i]) for i, (a, b) in enumerate(zip(ins, outs))]
    for copy in copies:
        copy.start()
    for copy in copies:
        copy.wait()


def chain_on_device(sizes, velocity_term, model_step, background, receivers, checkpoints):
    gxs, gys, gzs = sizes
    sx, sy, sz = model_step.shape
    nck, steps, nrec = background.shape[0], checkpoints.shape[0], receivers.shape[1]
    n, rows, lanes = gxs * gys * gzs, gxs * gys, sx * sy
    nz = sz * gzs // n
    per = sz // nz
    ext = 3 * nz
    blocks = steps // BLOCK
    halo = 2 * BLOCK
    dims = (gxs, gys, gzs, sx, sy, sz, nck, steps)
    f32 = jnp.float32
    dma = pltpu.SemaphoreType.DMA
    vmem = pl.BlockSpec(memory_space=pltpu.VMEM)
    hbm = pl.BlockSpec(memory_space=pltpu.HBM)
    tile = (2, gxs, lanes)
    shapes = (
        jax.ShapeDtypeStruct((sx, sy, sz), f32),
        jax.ShapeDtypeStruct((steps, nrec), f32),
        jax.ShapeDtypeStruct((sx, sy), f32),
        jax.ShapeDtypeStruct((sx, sy, sz), f32),
    )
    results = pl.pallas_call(
        functools.partial(chain_kernel, dims),
        out_shape=shapes,
        in_specs=[hbm] * 5,
        out_specs=(vmem,) * 4,
        scratch_shapes=[
            pltpu.VMEM(velocity_term.shape, f32),
            pltpu.VMEM(model_step.shape, f32),
            pltpu.VMEM(background.shape, background.dtype),
            pltpu.VMEM(receivers.shape, receivers.dtype),
            pltpu.SMEM(checkpoints.shape, checkpoints.dtype),
            pltpu.VMEM((per, (2 + nck) * nz, lanes), f32),
            pltpu.VMEM((rows * (2 + nck) * nz, lanes), f32),
            pltpu.VMEM((ext,) + tile, f32),
            pltpu.VMEM((nck, ext) + tile, f32),
            pltpu.VMEM((2, nck, halo // 2) + tile, f32),
            pltpu.VMEM((nck, nz) + tile, f32),
            pltpu.VMEM((steps, ext) + tile, f32),
            pltpu.VMEM((steps, ext) + tile, f32),
            pltpu.VMEM((ext,) + tile, f32),
            pltpu.VMEM((2 * lanes, 2 * lanes), jnp.bfloat16),
            pltpu.VMEM((ext * rows, 2 * lanes), f32),
            pltpu.VMEM((nz,) + tile, f32),
            pltpu.VMEM((ext,) + tile, f32),
            pltpu.VMEM((2, steps, nrec), f32),
            pltpu.VMEM((4, steps, nrec), f32),
            pltpu.VMEM((n // 4, steps, nrec), f32),
            pltpu.VMEM((rows * nz, lanes), f32),
            pltpu.VMEM((rows * nz, lanes), f32),
            pltpu.VMEM((rows, 1, lanes), f32),
            pltpu.VMEM((per, nz, lanes), f32),
            pltpu.VMEM((per, nz, lanes), f32),
            pltpu.VMEM((n, 1, lanes), f32),
            dma((5,)),
            dma((per,)),
            dma((rows,)),
            dma((12,)),
            dma((12,)),
            dma((2 * blocks - 1, 2, 2)),
            dma((2 * blocks - 1, 2, 2)),
            dma((2, max(4, n // 4))),
            dma((2, max(4, n // 4))),
            dma((rows,)),
            dma((per,)),
            dma((rows,)),
            dma((per,)),
            dma((n,)),
            dma((n,)),
        ],
        compiler_params=pltpu.CompilerParams(
            collective_id=0, has_side_effects=True, vmem_limit_bytes=48 * 1024 * 1024
        ),
    )(*(
        pltpu.with_memory_space_constraint(a, pltpu.HBM)
        for a in (velocity_term, model_step, background, receivers, checkpoints)
    ))
    return pl.pallas_call(
        store_kernel,
        out_shape=shapes,
        in_specs=[vmem] * 4,
        out_specs=(hbm,) * 4,
        scratch_shapes=[dma((4,))],
        compiler_params=pltpu.CompilerParams(vmem_limit_bytes=1024 * 1024),
    )(*results)


def solution(mesh):
    gxs, gys, gzs = mesh.shape["gx"], mesh.shape["gy"], mesh.shape["gz"]
    n = gxs * gys * gzs

    def whole(velocity_term, model_step, background, receivers, checkpoints):
        nx, ny, depth = model_step.shape
        fits = (
            depth % (8 * n) == 0
            and depth // n == 2 * BLOCK
            and gxs == 8
            and gys == 2
            and n % 4 == 0
            and nx // gxs == 4
            and (nx // gxs) * (ny // gys) == 128
            and checkpoints.shape[0] == 4 * BLOCK
        )
        body = functools.partial(chain_on_device, (gxs, gys, gzs)) if fits else on_device
        return jax.shard_map(
            body,
            mesh=mesh,
            in_specs=(P("gx", "gy", "gz"), P("gx", "gy", "gz"), P(None, "gx", "gy", "gz"), P(), P()),
            out_specs=(P("gx", "gy", "gz"), P(), P("gx", "gy"), P("gx", "gy", "gz")),
            check_vma=False,
        )(velocity_term, model_step, background, receivers, checkpoints)

    return whole
```

```python
import functools

import jax
import jax.numpy as jnp
from jax import lax
from jax.experimental import pallas as pl
from jax.experimental.pallas import tpu as pltpu
from jax.sharding import PartitionSpec as P

near_coef = 4.0 / 3.0
far_coef = -1.0 / 12.0
center_coef = -2.5


def with_halo(block, sides, width, periodic):
    for axis, dim in sides:
        count = lax.axis_size(axis)
        forward = [(i, i + 1) for i in range(count - 1)]
        if periodic:
            forward.append((count - 1, 0))
        backward = [(target, source) for source, target in forward]
        low = lax.ppermute(
            lax.slice_in_dim(block, block.shape[dim] - width, None, axis=dim), axis, forward
        )
        high = lax.ppermute(lax.slice_in_dim(block, 0, width, axis=dim), axis, backward)
        block = jnp.concatenate([low, block, high], axis=dim)
    return block


def along(padded, dim):
    count = padded.shape[dim]
    first = lax.slice_in_dim(padded, 3, count - 1, axis=dim) + lax.slice_in_dim(
        padded, 1, count - 3, axis=dim
    )
    second = lax.slice_in_dim(padded, 4, count, axis=dim) + lax.slice_in_dim(
        padded, 0, count - 4, axis=dim
    )
    return near_coef * first + far_coef * second


def laplace(field):
    side = with_halo(field, (("gx", 0), ("gy", 1)), 2, True)
    deep = with_halo(field, (("gz", 2),), 2, False)
    x_pad = side[:, 2:-2, :]
    y_pad = side[2:-2, :, :]
    return 3.0 * center_coef * field + along(x_pad, 0) + along(y_pad, 1) + along(deep, 2)


def sample_row(samples, field, step, clip_x, clip_y, clip_z, inside):
    values = field[clip_x, clip_y, clip_z] * inside
    return lax.dynamic_update_index_in_dim(samples, values, step, 0)


def on_device(velocity_term, model_step, background, receivers, checkpoints):
    size_x, size_y, size_z = model_step.shape
    steps = checkpoints.shape[0]
    local_x = receivers[0] - lax.axis_index("gx") * size_x
    local_y = receivers[1] - lax.axis_index("gy") * size_y
    local_z = receivers[2] - lax.axis_index("gz") * size_z
    inside = (
        (local_x >= 0)
        & (local_x < size_x)
        & (local_y >= 0)
        & (local_y < size_y)
        & (local_z >= 0)
        & (local_z < size_z)
    )
    inside = inside.astype(jnp.float32)
    clip_x = jnp.clip(local_x, 0, size_x - 1)
    clip_y = jnp.clip(local_y, 0, size_y - 1)
    clip_z = jnp.clip(local_z, 0, size_z - 1)
    zeros = jnp.zeros(model_step.shape, jnp.float32)
    record = jnp.zeros((steps, receivers.shape[1]), jnp.float32)

    def forward(step, carry):
        previous, current, samples = carry
        accel = lax.dynamic_index_in_dim(background, checkpoints[step], 0, keepdims=False).astype(
            jnp.float32
        )
        following = 2.0 * current - previous + velocity_term * laplace(current) + model_step * accel
        samples = sample_row(samples, following, step, clip_x, clip_y, clip_z, inside)
        return (current, following, samples)

    previous, current, record = lax.fori_loop(0, steps, forward, (zeros, zeros, record))
    traces = lax.psum(record, ("gx", "gy", "gz"))

    def adjoint_step(back, carry):
        later_two, later, image = carry
        step = steps - 1 - back
        accel = lax.dynamic_index_in_dim(background, checkpoints[step], 0, keepdims=False).astype(
            jnp.float32
        )
        adjoint = 2.0 * later - later_two + laplace(velocity_term * later)
        inject = lax.dynamic_index_in_dim(traces, step, 0, keepdims=False) * inside
        adjoint = adjoint.at[clip_x, clip_y, clip_z].add(inject)
        return (later, adjoint, image + adjoint * accel)

    later_two, later, image = lax.fori_loop(0, steps, adjoint_step, (zeros, zeros, zeros))
    depth_total = size_z * lax.axis_size("gz")
    column_image = lax.psum(jnp.sum(image, axis=2), "gz") / depth_total
    return (image, traces, column_image, current)


MESH = pl.DeviceIdType.MESH
BLOCK = 4
GROUP = 4


def place_of(p, gxs, gys, gzs):
    q, gz = p // gzs, p % gzs
    per = 2 * gys
    zz, w = q // per, q % per
    w = w + (zz % 2) * (per - 1 - 2 * w)
    xx, yy = w // gys, w % gys
    return 2 * zz + xx, yy + xx * (gys - 1 - 2 * yy), gz


def position_of(gx, gy, gz, gxs, gys, gzs):
    per = 2 * gys
    zz, xx = gx // 2, gx % 2
    w = xx * gys + gy + xx * (gys - 1 - 2 * gy)
    w = w + (zz % 2) * (per - 1 - 2 * w)
    return (zz * per + w) * gzs + gz


def lane_roll(a, k):
    return pltpu.roll(a, k % a.shape[-1], a.ndim - 1)


def row_roll(a, k):
    return pltpu.roll(a, k % a.shape[-2], a.ndim - 2)


def quarter_owner(k, gy):
    base = (k % 2) * 2 + k // 2
    return base + gy * (2 - 4 * (k % 2))


class Plane:
    def __init__(self, rows, lanes):
        half = lanes // 2
        lane = lax.broadcasted_iota(jnp.int32, (rows, lanes), 1)
        self.half = half
        self.even = lane < half
        self.odd_quarter = lane % half >= half // 2

    def swap_quarters(self, a):
        quarter = self.half // 2
        return jnp.where(self.odd_quarter, lane_roll(a, quarter), lane_roll(a, -quarter))

    def join(self, low, high):
        return (
            jnp.where(self.odd_quarter, high, low),
            self.swap_quarters(jnp.where(self.odd_quarter, low, high)),
        )

    def split(self, f0, f1):
        t = self.swap_quarters(f1)
        return jnp.where(self.odd_quarter, t, f0), jnp.where(self.odd_quarter, f0, t)

    def taps(self):
        lanes = 2 * self.half
        shape = (2 * lanes, 2 * lanes)
        i, j = lax.broadcasted_iota(jnp.int32, shape, 0) % lanes, lax.broadcasted_iota(jnp.int32, shape, 1)
        across = (i - j + lanes) % lanes == self.half
        shift = (j - i + lanes) % self.half
        same = (i < self.half) == (j < self.half)
        near = same & ((shift == 1) | (shift == self.half - 1))
        far = same & ((shift == 2) | (shift == self.half - 2))
        beside = jnp.where(near, -16.0, 0.0) + jnp.where(far, 1.0, 0.0)
        return (jnp.where(j < lanes, beside, 0.0) + jnp.where(across, -16.0, 0.0)).astype(jnp.bfloat16)

    def lateral(self, f, y_sum, other):
        x0, x1, f0, f1 = other[:, 0], other[:, 1], f[:, 0], f[:, 1]
        low = jnp.where(self.even, row_roll(x1, 1), x1) + (f1 + row_roll(f1, 1))
        high = jnp.where(self.even, x0, row_roll(x0, -1)) + (f0 + row_roll(f0, -1))
        return y_sum + jnp.stack([low, high], axis=1)


def chain_kernel(
    dims, v_hbm, m_hbm, bg_hbm, rec_hbm, ck_hbm,
    image_ref, traces_ref, column_ref, wave_ref,
    v_in, m_in, bg_in, rec_in, ck_in,
    stage, landed, vel, src, far, own_bg, hist, adj, wbuf, taps, mixed, img, count, part, tr1, tr2,
    back_w, back_i, in_w, in_i, in_c,
    s_0, s_in, r_in, s_c, r_c, s_f, r_f, s_t, r_t, s_w, r_w, s_i, r_i, s_k, r_k,
):
    gxs, gys, gzs, sx, sy, sz, nck, steps = dims
    n = gxs * gys * gzs
    rows = gxs * gys
    lanes = sx * sy
    nz = sz * gzs // n
    per = sz // nz
    fields = 2 + nck
    gx, gy, gz = lax.axis_index("gx"), lax.axis_index("gy"), lax.axis_index("gz")
    pos = position_of(gx, gy, gz, gxs, gys, gzs)
    my_row = gx * gys + gy
    lo_id = place_of(jnp.maximum(pos - 1, 0), gxs, gys, gzs)
    hi_id = place_of(jnp.minimum(pos + 1, n - 1), gxs, gys, gzs)
    has_lo, has_hi = pos > 0, pos < n - 1
    ext = 3 * nz
    f32 = jnp.float32
    tile = (gxs, lanes)

    def remote(src_ref, dst_ref, ss, rs, where):
        return pltpu.make_async_remote_copy(
            src_ref=src_ref, dst_ref=dst_ref, send_sem=ss, recv_sem=rs, device_id=where, device_id_type=MESH
        )

    barrier = pltpu.get_barrier_semaphore()

    def greet(p, carry):
        @pl.when(p != pos)
        def _():
            pl.semaphore_signal(barrier, inc=1, device_id=place_of(p, gxs, gys, gzs), device_id_type=MESH)
        return carry

    loads = [
        pltpu.make_async_copy(a, b, s_0.at[i])
        for i, (a, b) in enumerate(
            ((v_hbm, v_in), (m_hbm, m_in), (bg_hbm, bg_in), (rec_hbm, rec_in), (ck_hbm, ck_in))
        )
    ]
    for load in loads:
        load.start()
    lax.fori_loop(0, n, greet, 0)

    plane = Plane(gxs, lanes)

    @pl.when(jnp.logical_not(has_lo))
    def _():
        vel[0:nz] = jnp.zeros((nz, 2) + tile, f32)
        for k in range(nck):
            src[k, 0:nz] = jnp.zeros((nz, 2) + tile, f32)
        for t in range(steps):
            hist[t, 0:nz] = jnp.zeros((nz, 2) + tile, f32)
            adj[t, 0:nz] = jnp.zeros((nz, 2) + tile, f32)

    @pl.when(jnp.logical_not(has_hi))
    def _():
        vel[2 * nz :] = jnp.zeros((nz, 2) + tile, f32)
        for k in range(nck):
            src[k, 2 * nz :] = jnp.zeros((nz, 2) + tile, f32)
        for t in range(steps):
            hist[t, 2 * nz :] = jnp.zeros((nz, 2) + tile, f32)
            adj[t, 2 * nz :] = jnp.zeros((nz, 2) + tile, f32)

    for load in loads[:3]:
        load.wait()
    for f in range(fields):
        pieces = []
        for k in range(sx):
            x = quarter_owner(k, gy)
            if f == 0:
                pieces.append(v_in[x])
            elif f == 1:
                pieces.append(m_in[x])
            else:
                pieces.append(bg_in[f - 2, x].astype(f32))
        turned = jnp.concatenate(pieces, axis=0).T
        stage[:, f * nz : (f + 1) * nz, :] = turned.reshape(per, nz, lanes)
    pl.semaphore_wait(barrier, n - 1)

    slab = fields * nz

    def arrival(row):
        return landed.at[pl.ds(pl.multiple_of(row * slab, nz), slab)]

    def scatter_in(i, carry):
        c = lax.rem(i + my_row, per)
        p = gz * per + c

        @pl.when(p != pos)
        def _():
            remote(stage.at[c], arrival(my_row), s_in.at[c], r_in.at[my_row], place_of(p, gxs, gys, gzs)).start()

        @pl.when(p == pos)
        def _():
            landed[pl.ds(pl.multiple_of(my_row * slab, nz), slab), :] = stage[c]

        return carry

    lax.fori_loop(0, per, scatter_in, 0)

    for load in loads[3:]:
        load.wait()
    rec = rec_in[...]
    rx, ry, rz = rec[0:1], rec[1:2], rec[2:3]
    nrec = rec.shape[1]
    rlane = (rx % 2) * (lanes // 2) + ry
    rlocal = rz - (pos - 1) * nz
    zr = jnp.where((rlocal >= 0) & (rlocal < ext), (rlocal * 2 + (rx % sx) // 2) * gxs + rx // sx, -1)
    one_zr = (lax.broadcasted_iota(jnp.int32, (ext * rows, nrec), 0) == zr).astype(f32)
    one_lane = (lax.broadcasted_iota(jnp.int32, (lanes, nrec), 0) == rlane).astype(f32)
    counted = lax.dot_general(
        one_zr.astype(jnp.bfloat16), one_lane.astype(jnp.bfloat16), (((1,), (1,)), ((), ())),
        preferred_element_type=f32,
    )
    count[...] = counted.reshape((ext, 2) + tile)
    img[...] = jnp.zeros_like(img)
    taps[...] = plane.taps()

    owner = pos // per

    def wait_in(row, carry):
        sender = row // gys, row % gys, owner

        @pl.when((row != my_row) | (owner != gz))
        def _():
            remote(stage.at[0], arrival(row), s_in.at[0], r_in.at[row], sender).wait_recv()

        return carry

    lax.fori_loop(0, rows, wait_in, 0)

    def gathered(f, z):
        low = landed[pl.ds(f * nz + z, gxs, stride=gys * slab), :]
        high = landed[pl.ds(slab + f * nz + z, gxs, stride=gys * slab), :]
        return plane.join(low, high)

    for z in range(nz):
        vs = gathered(0, z)
        ms = gathered(1, z)
        for c in range(2):
            vel[nz + z, c] = far_coef * vs[c]
        for k in range(nck):
            accel = gathered(2 + k, z)
            for c in range(2):
                own_bg[k, z, c] = accel[c]
                src[k, nz + z, c] = ms[c] * accel[c]

    halo = 2 * BLOCK
    soon, rest = halo // 4, halo // 2

    def pairs(make):
        return make(0, lo_id), make(1, hi_id)

    def ranges(side, near_at, size):
        at = nz - near_at - size if side else near_at
        return pl.ds(nz + at, size), pl.ds(at if side else 2 * nz + at, size)

    def first_coefs(side, where):
        a, b = ranges(side, 0, soon)
        c, d = ranges(side, soon, soon)
        i = 3 * side
        j = 3 * (1 - side)
        return [
            remote(src.at[0, c], src.at[0, d], s_c.at[i], r_c.at[j], where),
            remote(src.at[:, a], src.at[:, b], s_c.at[i + 1], r_c.at[j + 1], where),
            remote(vel.at[a], vel.at[b], s_c.at[i + 2], r_c.at[j + 2], where),
        ]

    def later_coefs(side, where):
        a, b = ranges(side, soon, halo - soon)
        c, _ = ranges(side, 2 * soon, soon)
        d, _ = ranges(side, soon, rest)
        i = 6 + 3 * side
        j = 6 + 3 * (1 - side)
        return [
            remote(src.at[0, c], far.at[1 - side, 0, pl.ds(0, soon)], s_c.at[i], r_c.at[j], where),
            remote(src.at[pl.ds(1, nck - 1), d], far.at[1 - side, pl.ds(1, nck - 1)], s_c.at[i + 1], r_c.at[j + 1], where),
            remote(vel.at[a], vel.at[b], s_c.at[i + 2], r_c.at[j + 2], where),
        ]

    def newer_copies(e, newer):
        def make(side, where):
            a, b = ranges(side, 0, nz)
            return [remote(newer.at[a], newer.at[b], s_f.at[e, side, 0], r_f.at[e, 1 - side, 0], where)]
        return pairs(make)

    def older_copies(e, older):
        def make(side, where):
            a, b = ranges(side, 2, halo - 4)
            return [remote(older.at[a], older.at[b], s_f.at[e, side, 1], r_f.at[e, 1 - side, 1], where)]
        return pairs(make)

    def launch(copies):
        to_lo, to_hi = copies

        @pl.when(has_hi)
        def _():
            for c in to_hi:
                c.start()

        @pl.when(has_lo)
        def _():
            for c in to_lo:
                c.start()

    def settle(copies):
        to_lo, to_hi = copies

        @pl.when(has_hi)
        def _():
            for c in to_lo:
                c.wait_recv()
            for c in to_hi:
                c.wait_send()

        @pl.when(has_lo)
        def _():
            for c in to_hi:
                c.wait_recv()
            for c in to_lo:
                c.wait_send()

    opening, closing = pairs(first_coefs), pairs(later_coefs)
    launch(opening)
    launch(closing)

    def sent_in(c, carry):
        @pl.when(gz * per + c != pos)
        def _():
            remote(stage.at[c], arrival(my_row), s_in.at[c], r_in.at[my_row], lo_id).wait_send()

        return carry

    lax.fori_loop(0, per, sent_in, 0)
    settle(opening)

    def lateral_sums(ref, width):
        size = nz + 2 * width
        f = ref[pl.ds(nz - width, size)].reshape(size * rows, lanes)
        top = f.astype(jnp.bfloat16)
        low = (f - top.astype(f32)).astype(jnp.bfloat16)
        mixed[pl.ds((nz - width) * rows, size * rows)] = jnp.dot(
            jnp.concatenate([top, low], axis=1), taps[...], preferred_element_type=f32
        )

    def spread(ref, at, size):
        f = ref[pl.ds(at, size)]
        m = pl.ds(at * rows, size * rows)
        shape = (size, 2) + tile
        near = ref[pl.ds(at + 1, size)] + ref[pl.ds(at - 1, size)]
        wide = ref[pl.ds(at + 2, size)] + ref[pl.ds(at - 2, size)]
        flat = plane.lateral(f, mixed[m, 0:lanes].reshape(shape), mixed[m, lanes : 2 * lanes].reshape(shape))
        return flat + wide - 16.0 * near + 90.0 * f, f

    def groups(width):
        lo, hi = nz - width, 2 * nz + width
        for at in range(lo, hi, GROUP):
            yield at, min(GROUP, hi - at)

    def forward_step(t, width):
        k = ck_in[t]
        lateral_sums(hist.at[t - 1], width)
        for at, size in groups(width):
            here = pl.ds(at, size)
            lap, f = spread(hist.at[t - 1], at, size)
            value = 2.0 * f + vel[here] * lap + src[k, here]
            if t > 1:
                value = value - hist[t - 2, here]
            hist[t, here] = value

    def adjoint_step(t, width):
        k = ck_in[t]
        first = t == steps - 1
        if not first:
            for at, size in groups(width + 2):
                here = pl.ds(at, size)
                wbuf[here] = vel[here] * adj[t + 1, here]
            lateral_sums(wbuf, width)
        for at, size in groups(width):
            here = pl.ds(at, size)
            value = count[here] * hist[t, here]
            if not first:
                lap, _ = spread(wbuf, at, size)
                value = value + lap + 2.0 * adj[t + 1, here]
                if t < steps - 2:
                    value = value - adj[t + 2, here]
            adj[t, here] = value
        img[...] = img[...] + adj[t, nz : 2 * nz] * own_bg[k]

    blocks = steps // BLOCK

    for z in range(nz - 2 * soon, 2 * nz + 2 * soon):
        for c in range(2):
            hist[0, z, c] = src[0, z, c]
    forward_step(1, 2)
    older = older_copies(0, hist.at[1])
    launch(older)
    forward_step(2, 0)
    newer = newer_copies(0, hist.at[2])
    launch(newer)
    settle(closing)

    @pl.when(has_lo)
    def _():
        src[0, nz - halo + 2 : nz - halo + 2 + soon] = far[0, 0, 0:soon]
        src[1:, nz - halo + 2 : nz - soon] = far[0, 1:]

    @pl.when(has_hi)
    def _():
        src[0, 2 * nz + 2 * soon : 2 * nz + 3 * soon] = far[1, 0, 0:soon]
        src[1:, 2 * nz + soon : 2 * nz + 3 * soon] = far[1, 1:]

    settle(older)
    settle(newer)

    def forward_block(b):
        t = b * BLOCK - 1
        for j in range(BLOCK - 1):
            forward_step(t + j, halo - 2 * (j + 1))
        older = older_copies(b, hist.at[t + BLOCK - 2])
        launch(older)
        forward_step(t + BLOCK - 1, 0)
        newer = newer_copies(b, hist.at[t + BLOCK - 1])
        launch(newer)
        settle(older)
        settle(newer)

    for b in range(1, blocks):
        forward_block(b)

    def send_back(src_ref, dst, ss, rs, slot, g):
        def one(i, carry):
            row = lax.rem(my_row + rows // 2 + i, rows)
            other = (row != my_row) | (g != gz)
            piece = src_ref.at[pl.ds(pl.multiple_of(row * nz, nz), nz)]

            @pl.when(other)
            def _():
                remote(piece, dst.at[slot], ss.at[row], rs.at[slot], (row // gys, row % gys, g)).start()

            @pl.when(jnp.logical_not(other))
            def _():
                dst[slot] = piece[...]

            return carry

        lax.fori_loop(0, rows, one, 0)

    def sent_back(src_ref, dst, ss, rs, g):
        def one(row, carry):
            @pl.when((row != my_row) | (g != gz))
            def _():
                remote(src_ref.at[pl.ds(0, nz)], dst.at[0], ss.at[row], rs.at[0], lo_id).wait_send()

            return carry

        lax.fori_loop(0, rows, one, 0)

    def got_back(src_ref, dst, ss, rs, first, number):
        def one(c, carry):
            @pl.when(c + first != pos)
            def _():
                remote(src_ref.at[pl.ds(0, nz)], dst.at[c], ss.at[0], rs.at[c], lo_id).wait_recv()

            return carry

        lax.fori_loop(0, number, one, 0)

    near = 4
    apart = n // near
    team, seat = pos // near, pos % near

    def trace_sends(src_ref, dst, kind):
        number = near if kind == 0 else apart
        mine = seat if kind == 0 else team

        def one(i, carry):
            @pl.when(i != mine)
            def _():
                p = team * near + i if kind == 0 else i * near + seat
                remote(src_ref, dst.at[mine], s_t.at[kind, i], r_t.at[kind, mine], place_of(p, gxs, gys, gzs)).start()

            return carry

        lax.fori_loop(0, number, one, 0)

    def trace_waits(src_ref, dst, kind):
        number = near if kind == 0 else apart
        mine = seat if kind == 0 else team

        def one(i, carry):
            @pl.when(i != mine)
            def _():
                remote(src_ref, dst.at[i], s_t.at[kind, i], r_t.at[kind, i], lo_id).wait()

            return carry

        lax.fori_loop(0, number, one, 0)

    def gather_traces():
        picked = one_zr[nz * rows : 2 * nz * rows]
        lane_pick = one_lane.astype(jnp.bfloat16)
        lines = []
        for t in range(steps):
            table = hist[t, nz : 2 * nz].reshape(nz * rows, lanes)
            at_row = jnp.zeros((nz * rows, nrec), f32)
            for _ in range(3):
                piece = table.astype(jnp.bfloat16)
                at_row = at_row + jnp.dot(piece, lane_pick, preferred_element_type=f32)
                table = table - piece.astype(f32)
            lines.append(jnp.sum(at_row * picked, axis=0, keepdims=True))
        return jnp.concatenate(lines, axis=0)

    def give_back(read, dst):
        for z in range(nz):
            for g, value in enumerate(plane.split(*read(z))):
                dst[pl.ds(g * nz + z, gxs, stride=gys * nz), :] = value

    last = steps - 1
    forward_step(last, halo - 2)
    adjoint_step(last, halo - 2)
    adjoint_step(last - 1, halo - 4)
    adjoint_step(last - 2, halo - 6)
    older = older_copies(blocks, adj.at[last - 2])
    launch(older)
    adjoint_step(last - 3, 0)
    newer = newer_copies(blocks, adj.at[last - 3])
    launch(newer)
    give_back(lambda z: (hist[last, nz + z, 0], hist[last, nz + z, 1]), back_w)
    send_back(back_w, in_w, s_w, r_w, lax.rem(pos, per), owner)
    part[0] = gather_traces()
    tr1[seat] = part[0]
    trace_sends(part.at[0], tr1, 0)
    settle(older)
    settle(newer)

    def trace_relay():
        trace_waits(part.at[0], tr1, 0)
        total = tr1[0]
        for i in range(1, near):
            total = total + tr1[i]
        part[1] = total
        tr2[team] = total
        trace_sends(part.at[1], tr2, 1)

    def adjoint_block(b):
        t = last - BLOCK * b
        for j in range(BLOCK - 1):
            adjoint_step(t - j, halo - 2 * (j + 1))
        if b == blocks - 1:
            adjoint_step(t - BLOCK + 1, 0)
            return
        older = older_copies(blocks + b, adj.at[t - BLOCK + 2])
        launch(older)
        adjoint_step(t - BLOCK + 1, 0)
        newer = newer_copies(blocks + b, adj.at[t - BLOCK + 1])
        launch(newer)
        if b == 1:
            trace_relay()
        settle(older)
        settle(newer)

    for b in range(1, blocks):
        adjoint_block(b)

    give_back(lambda z: (img[z, 0], img[z, 1]), back_i)
    send_back(back_i, in_i, s_i, r_i, lax.rem(pos, per), owner)
    trace_waits(part.at[1], tr2, 1)
    total = tr2[0]
    for i in range(1, apart):
        total = total + tr2[i]
    traces_ref[...] = total

    def put_out(buffer, out_ref):
        turned = buffer[...].reshape(sz, lanes).T
        for k in range(sx):
            out_ref[quarter_owner(k, gy)] = turned[k * sy : (k + 1) * sy]

    got_back(back_w, in_w, s_w, r_w, gz * per, per)
    put_out(in_w, wave_ref)
    sent_back(back_w, in_w, s_w, r_w, owner)
    sent_back(back_i, in_i, s_i, r_i, owner)

    got_back(back_i, in_i, s_i, r_i, gz * per, per)
    in_c[gz] = jnp.sum(in_i[...].reshape(sz, lanes), axis=0, keepdims=True)

    def sums_to(i, where):
        return remote(in_c.at[gz], in_c.at[gz], s_k.at[i], r_k.at[gz], (gx, gy, where))

    def sums_from(i):
        return remote(in_c.at[i], in_c.at[i], s_k.at[i], r_k.at[i], (gx, gy, i))

    for step in range(1, gzs):
        sums_to(step, lax.rem(gz + step, gzs)).start()
    put_out(in_i, image_ref)
    for step in range(1, gzs):
        sums_from(lax.rem(gz + step, gzs)).wait_recv()
    depth = in_c[0]
    for i in range(1, gzs):
        depth = depth + in_c[i]
    depth = depth / (sz * gzs)
    for k in range(sx):
        column_ref[pl.ds(quarter_owner(k, gy), 1), :] = depth[:, k * sy : (k + 1) * sy]
    for step in range(1, gzs):
        sums_to(step, lax.rem(gz + step, gzs)).wait_send()


def store_kernel(*refs):
    count = len(refs) // 2
    ins, outs, sems = refs[:count], refs[count : 2 * count], refs[2 * count]
    copies = [pltpu.make_async_copy(a, b, sems.at[i]) for i, (a, b) in enumerate(zip(ins, outs))]
    for copy in copies:
        copy.start()
    for copy in copies:
        copy.wait()


def chain_on_device(sizes, velocity_term, model_step, background, receivers, checkpoints):
    gxs, gys, gzs = sizes
    sx, sy, sz = model_step.shape
    nck, steps, nrec = background.shape[0], checkpoints.shape[0], receivers.shape[1]
    n, rows, lanes = gxs * gys * gzs, gxs * gys, sx * sy
    nz = sz * gzs // n
    per = sz // nz
    ext = 3 * nz
    blocks = steps // BLOCK
    halo = 2 * BLOCK
    dims = (gxs, gys, gzs, sx, sy, sz, nck, steps)
    f32 = jnp.float32
    dma = pltpu.SemaphoreType.DMA
    vmem = pl.BlockSpec(memory_space=pltpu.VMEM)
    hbm = pl.BlockSpec(memory_space=pltpu.HBM)
    tile = (2, gxs, lanes)
    shapes = (
        jax.ShapeDtypeStruct((sx, sy, sz), f32),
        jax.ShapeDtypeStruct((steps, nrec), f32),
        jax.ShapeDtypeStruct((sx, sy), f32),
        jax.ShapeDtypeStruct((sx, sy, sz), f32),
    )
    results = pl.pallas_call(
        functools.partial(chain_kernel, dims),
        out_shape=shapes,
        in_specs=[hbm] * 5,
        out_specs=(vmem,) * 4,
        scratch_shapes=[
            pltpu.VMEM(velocity_term.shape, f32),
            pltpu.VMEM(model_step.shape, f32),
            pltpu.VMEM(background.shape, background.dtype),
            pltpu.VMEM(receivers.shape, receivers.dtype),
            pltpu.SMEM(checkpoints.shape, checkpoints.dtype),
            pltpu.VMEM((per, (2 + nck) * nz, lanes), f32),
            pltpu.VMEM((rows * (2 + nck) * nz, lanes), f32),
            pltpu.VMEM((ext,) + tile, f32),
            pltpu.VMEM((nck, ext) + tile, f32),
            pltpu.VMEM((2, nck, halo // 2) + tile, f32),
            pltpu.VMEM((nck, nz) + tile, f32),
            pltpu.VMEM((steps, ext) + tile, f32),
            pltpu.VMEM((steps, ext) + tile, f32),
            pltpu.VMEM((ext,) + tile, f32),
            pltpu.VMEM((2 * lanes, 2 * lanes), jnp.bfloat16),
            pltpu.VMEM((ext * rows, 2 * lanes), f32),
            pltpu.VMEM((nz,) + tile, f32),
            pltpu.VMEM((ext,) + tile, f32),
            pltpu.VMEM((2, steps, nrec), f32),
            pltpu.VMEM((4, steps, nrec), f32),
            pltpu.VMEM((n // 4, steps, nrec), f32),
            pltpu.VMEM((rows * nz, lanes), f32),
            pltpu.VMEM((rows * nz, lanes), f32),
            pltpu.VMEM((per, nz, lanes), f32),
            pltpu.VMEM((per, nz, lanes), f32),
            pltpu.VMEM((gzs, 1, lanes), f32),
            dma((5,)),
            dma((per,)),
            dma((rows,)),
            dma((12,)),
            dma((12,)),
            dma((2 * blocks - 1, 2, 2)),
            dma((2 * blocks - 1, 2, 2)),
            dma((2, max(4, n // 4))),
            dma((2, max(4, n // 4))),
            dma((rows,)),
            dma((per,)),
            dma((rows,)),
            dma((per,)),
            dma((gzs,)),
            dma((gzs,)),
        ],
        compiler_params=pltpu.CompilerParams(
            collective_id=0, has_side_effects=True, vmem_limit_bytes=48 * 1024 * 1024
        ),
    )(*(
        pltpu.with_memory_space_constraint(a, pltpu.HBM)
        for a in (velocity_term, model_step, background, receivers, checkpoints)
    ))
    return pl.pallas_call(
        store_kernel,
        out_shape=shapes,
        in_specs=[vmem] * 4,
        out_specs=(hbm,) * 4,
        scratch_shapes=[dma((4,))],
        compiler_params=pltpu.CompilerParams(vmem_limit_bytes=1024 * 1024),
    )(*results)


def solution(mesh):
    gxs, gys, gzs = mesh.shape["gx"], mesh.shape["gy"], mesh.shape["gz"]
    n = gxs * gys * gzs

    def whole(velocity_term, model_step, background, receivers, checkpoints):
        nx, ny, depth = model_step.shape
        fits = (
            depth % (8 * n) == 0
            and depth // n == 2 * BLOCK
            and gxs == 8
            and gys == 2
            and n % 4 == 0
            and nx // gxs == 4
            and (nx // gxs) * (ny // gys) == 128
            and checkpoints.shape[0] == 4 * BLOCK
        )
        body = functools.partial(chain_on_device, (gxs, gys, gzs)) if fits else on_device
        return jax.shard_map(
            body,
            mesh=mesh,
            in_specs=(P("gx", "gy", "gz"), P("gx", "gy", "gz"), P(None, "gx", "gy", "gz"), P(), P()),
            out_specs=(P("gx", "gy", "gz"), P(), P("gx", "gy"), P("gx", "gy", "gz")),
            check_vma=False,
        )(velocity_term, model_step, background, receivers, checkpoints)

    return whole
```

```python
import functools

import jax
import jax.numpy as jnp
from jax import lax
from jax.experimental import pallas as pl
from jax.experimental.pallas import tpu as pltpu
from jax.sharding import PartitionSpec as P

near_coef = 4.0 / 3.0
far_coef = -1.0 / 12.0
center_coef = -2.5


def with_halo(block, sides, width, periodic):
    for axis, dim in sides:
        count = lax.axis_size(axis)
        forward = [(i, i + 1) for i in range(count - 1)]
        if periodic:
            forward.append((count - 1, 0))
        backward = [(target, source) for source, target in forward]
        low = lax.ppermute(
            lax.slice_in_dim(block, block.shape[dim] - width, None, axis=dim), axis, forward
        )
        high = lax.ppermute(lax.slice_in_dim(block, 0, width, axis=dim), axis, backward)
        block = jnp.concatenate([low, block, high], axis=dim)
    return block


def along(padded, dim):
    count = padded.shape[dim]
    first = lax.slice_in_dim(padded, 3, count - 1, axis=dim) + lax.slice_in_dim(
        padded, 1, count - 3, axis=dim
    )
    second = lax.slice_in_dim(padded, 4, count, axis=dim) + lax.slice_in_dim(
        padded, 0, count - 4, axis=dim
    )
    return near_coef * first + far_coef * second


def laplace(field):
    side = with_halo(field, (("gx", 0), ("gy", 1)), 2, True)
    deep = with_halo(field, (("gz", 2),), 2, False)
    x_pad = side[:, 2:-2, :]
    y_pad = side[2:-2, :, :]
    return 3.0 * center_coef * field + along(x_pad, 0) + along(y_pad, 1) + along(deep, 2)


def sample_row(samples, field, step, clip_x, clip_y, clip_z, inside):
    values = field[clip_x, clip_y, clip_z] * inside
    return lax.dynamic_update_index_in_dim(samples, values, step, 0)


def on_device(velocity_term, model_step, background, receivers, checkpoints):
    size_x, size_y, size_z = model_step.shape
    steps = checkpoints.shape[0]
    local_x = receivers[0] - lax.axis_index("gx") * size_x
    local_y = receivers[1] - lax.axis_index("gy") * size_y
    local_z = receivers[2] - lax.axis_index("gz") * size_z
    inside = (
        (local_x >= 0)
        & (local_x < size_x)
        & (local_y >= 0)
        & (local_y < size_y)
        & (local_z >= 0)
        & (local_z < size_z)
    )
    inside = inside.astype(jnp.float32)
    clip_x = jnp.clip(local_x, 0, size_x - 1)
    clip_y = jnp.clip(local_y, 0, size_y - 1)
    clip_z = jnp.clip(local_z, 0, size_z - 1)
    zeros = jnp.zeros(model_step.shape, jnp.float32)
    record = jnp.zeros((steps, receivers.shape[1]), jnp.float32)

    def forward(step, carry):
        previous, current, samples = carry
        accel = lax.dynamic_index_in_dim(background, checkpoints[step], 0, keepdims=False).astype(
            jnp.float32
        )
        following = 2.0 * current - previous + velocity_term * laplace(current) + model_step * accel
        samples = sample_row(samples, following, step, clip_x, clip_y, clip_z, inside)
        return (current, following, samples)

    previous, current, record = lax.fori_loop(0, steps, forward, (zeros, zeros, record))
    traces = lax.psum(record, ("gx", "gy", "gz"))

    def adjoint_step(back, carry):
        later_two, later, image = carry
        step = steps - 1 - back
        accel = lax.dynamic_index_in_dim(background, checkpoints[step], 0, keepdims=False).astype(
            jnp.float32
        )
        adjoint = 2.0 * later - later_two + laplace(velocity_term * later)
        inject = lax.dynamic_index_in_dim(traces, step, 0, keepdims=False) * inside
        adjoint = adjoint.at[clip_x, clip_y, clip_z].add(inject)
        return (later, adjoint, image + adjoint * accel)

    later_two, later, image = lax.fori_loop(0, steps, adjoint_step, (zeros, zeros, zeros))
    depth_total = size_z * lax.axis_size("gz")
    column_image = lax.psum(jnp.sum(image, axis=2), "gz") / depth_total
    return (image, traces, column_image, current)


MESH = pl.DeviceIdType.MESH
BLOCK = 4
GROUP = 4


def place_of(p, gxs, gys, gzs):
    q, gz = p // gzs, p % gzs
    per = 2 * gys
    zz, w = q // per, q % per
    w = w + (zz % 2) * (per - 1 - 2 * w)
    xx, yy = w // gys, w % gys
    return 2 * zz + xx, yy + xx * (gys - 1 - 2 * yy), gz


def position_of(gx, gy, gz, gxs, gys, gzs):
    per = 2 * gys
    zz, xx = gx // 2, gx % 2
    w = xx * gys + gy + xx * (gys - 1 - 2 * gy)
    w = w + (zz % 2) * (per - 1 - 2 * w)
    return (zz * per + w) * gzs + gz


def lane_roll(a, k):
    return pltpu.roll(a, k % a.shape[-1], a.ndim - 1)


def row_roll(a, k):
    return pltpu.roll(a, k % a.shape[-2], a.ndim - 2)


def quarter_owner(k, gy):
    base = (k % 2) * 2 + k // 2
    return base + gy * (2 - 4 * (k % 2))


class Plane:
    def __init__(self, rows, lanes):
        half = lanes // 2
        lane = lax.broadcasted_iota(jnp.int32, (rows, lanes), 1)
        self.half = half
        self.even = lane < half
        self.odd_quarter = lane % half >= half // 2

    def swap_quarters(self, a):
        quarter = self.half // 2
        return jnp.where(self.odd_quarter, lane_roll(a, quarter), lane_roll(a, -quarter))

    def join(self, low, high):
        return (
            jnp.where(self.odd_quarter, high, low),
            self.swap_quarters(jnp.where(self.odd_quarter, low, high)),
        )

    def split(self, f0, f1):
        t = self.swap_quarters(f1)
        return jnp.where(self.odd_quarter, t, f0), jnp.where(self.odd_quarter, f0, t)

    def taps(self):
        lanes = 2 * self.half
        shape = (2 * lanes, 2 * lanes)
        i, j = lax.broadcasted_iota(jnp.int32, shape, 0) % lanes, lax.broadcasted_iota(jnp.int32, shape, 1)
        across = (i - j + lanes) % lanes == self.half
        shift = (j - i + lanes) % self.half
        same = (i < self.half) == (j < self.half)
        near = same & ((shift == 1) | (shift == self.half - 1))
        far = same & ((shift == 2) | (shift == self.half - 2))
        beside = jnp.where(near, -16.0, 0.0) + jnp.where(far, 1.0, 0.0)
        return (jnp.where(j < lanes, beside, 0.0) + jnp.where(across, -16.0, 0.0)).astype(jnp.bfloat16)

    def lateral(self, f, y_sum, other):
        x0, x1, f0, f1 = other[:, 0], other[:, 1], f[:, 0], f[:, 1]
        low = jnp.where(self.even, row_roll(x1, 1), x1) + (f1 + row_roll(f1, 1))
        high = jnp.where(self.even, x0, row_roll(x0, -1)) + (f0 + row_roll(f0, -1))
        return y_sum + jnp.stack([low, high], axis=1)


def chain_kernel(
    dims, v_hbm, m_hbm, bg_hbm, rec_hbm, ck_hbm,
    image_ref, traces_ref, column_ref, wave_ref,
    v_in, m_in, bg_in, rec_in, ck_in,
    stage, landed, vel, src, far, own_bg, hist, adj, wbuf, taps, mixed, img, count, part, tr1, tr2,
    back_w, back_i, in_w, in_i, in_c,
    s_0, s_in, r_in, s_c, r_c, s_f, r_f, s_t, r_t, s_w, r_w, s_i, r_i, s_k, r_k,
):
    gxs, gys, gzs, sx, sy, sz, nck, steps = dims
    n = gxs * gys * gzs
    rows = gxs * gys
    lanes = sx * sy
    nz = sz * gzs // n
    per = sz // nz
    fields = 2 + nck
    gx, gy, gz = lax.axis_index("gx"), lax.axis_index("gy"), lax.axis_index("gz")
    pos = position_of(gx, gy, gz, gxs, gys, gzs)
    my_row = gx * gys + gy
    lo_id = place_of(jnp.maximum(pos - 1, 0), gxs, gys, gzs)
    hi_id = place_of(jnp.minimum(pos + 1, n - 1), gxs, gys, gzs)
    has_lo, has_hi = pos > 0, pos < n - 1
    ext = 3 * nz
    f32 = jnp.float32
    tile = (gxs, lanes)

    def remote(src_ref, dst_ref, ss, rs, where):
        return pltpu.make_async_remote_copy(
            src_ref=src_ref, dst_ref=dst_ref, send_sem=ss, recv_sem=rs, device_id=where, device_id_type=MESH
        )

    barrier = pltpu.get_barrier_semaphore()

    def greet(p, carry):
        @pl.when(p != pos)
        def _():
            pl.semaphore_signal(barrier, inc=1, device_id=place_of(p, gxs, gys, gzs), device_id_type=MESH)
        return carry

    loads = [
        pltpu.make_async_copy(a, b, s_0.at[i])
        for i, (a, b) in enumerate(
            ((v_hbm, v_in), (m_hbm, m_in), (bg_hbm, bg_in), (rec_hbm, rec_in), (ck_hbm, ck_in))
        )
    ]
    for load in loads:
        load.start()
    lax.fori_loop(0, n, greet, 0)

    plane = Plane(gxs, lanes)

    @pl.when(jnp.logical_not(has_lo))
    def _():
        vel[0:nz] = jnp.zeros((nz, 2) + tile, f32)
        for k in range(nck):
            src[k, 0:nz] = jnp.zeros((nz, 2) + tile, f32)
        for t in range(steps):
            hist[t, 0:nz] = jnp.zeros((nz, 2) + tile, f32)
            adj[t, 0:nz] = jnp.zeros((nz, 2) + tile, f32)

    @pl.when(jnp.logical_not(has_hi))
    def _():
        vel[2 * nz :] = jnp.zeros((nz, 2) + tile, f32)
        for k in range(nck):
            src[k, 2 * nz :] = jnp.zeros((nz, 2) + tile, f32)
        for t in range(steps):
            hist[t, 2 * nz :] = jnp.zeros((nz, 2) + tile, f32)
            adj[t, 2 * nz :] = jnp.zeros((nz, 2) + tile, f32)

    for load in loads[:3]:
        load.wait()
    for f in range(fields):
        pieces = []
        for k in range(sx):
            x = quarter_owner(k, gy)
            if f == 0:
                pieces.append(v_in[x])
            elif f == 1:
                pieces.append(m_in[x])
            else:
                pieces.append(bg_in[f - 2, x].astype(f32))
        turned = jnp.concatenate(pieces, axis=0).T
        stage[:, f * nz : (f + 1) * nz, :] = turned.reshape(per, nz, lanes)
    pl.semaphore_wait(barrier, n - 1)

    slab = fields * nz

    def arrival(row):
        return landed.at[pl.ds(pl.multiple_of(row * slab, nz), slab)]

    def scatter_in(i, carry):
        c = lax.rem(i + my_row, per)
        p = gz * per + c

        @pl.when(p != pos)
        def _():
            remote(stage.at[c], arrival(my_row), s_in.at[c], r_in.at[my_row], place_of(p, gxs, gys, gzs)).start()

        @pl.when(p == pos)
        def _():
            landed[pl.ds(pl.multiple_of(my_row * slab, nz), slab), :] = stage[c]

        return carry

    lax.fori_loop(0, per, scatter_in, 0)

    for load in loads[3:]:
        load.wait()
    rec = rec_in[...]
    rx, ry, rz = rec[0:1], rec[1:2], rec[2:3]
    nrec = rec.shape[1]
    rlane = (rx % 2) * (lanes // 2) + ry
    rlocal = rz - (pos - 1) * nz
    zr = jnp.where((rlocal >= 0) & (rlocal < ext), (rlocal * 2 + (rx % sx) // 2) * gxs + rx // sx, -1)
    one_zr = (lax.broadcasted_iota(jnp.int32, (ext * rows, nrec), 0) == zr).astype(f32)
    one_lane = (lax.broadcasted_iota(jnp.int32, (lanes, nrec), 0) == rlane).astype(f32)
    counted = lax.dot_general(
        one_zr.astype(jnp.bfloat16), one_lane.astype(jnp.bfloat16), (((1,), (1,)), ((), ())),
        preferred_element_type=f32,
    )
    count[...] = counted.reshape((ext, 2) + tile)
    img[...] = jnp.zeros_like(img)
    taps[...] = plane.taps()

    owner = pos // per

    def wait_in(row, carry):
        sender = row // gys, row % gys, owner

        @pl.when((row != my_row) | (owner != gz))
        def _():
            remote(stage.at[0], arrival(row), s_in.at[0], r_in.at[row], sender).wait_recv()

        return carry

    lax.fori_loop(0, rows, wait_in, 0)

    def gathered(f):
        low, high = (
            jnp.stack([landed[pl.ds(g * slab + f * nz + z, gxs, stride=gys * slab), :] for z in range(nz)])
            for g in range(gys)
        )
        return plane.join(low, high)

    own = slice(nz, 2 * nz)
    vs, ms = gathered(0), gathered(1)
    for c in range(2):
        vel[own, c] = far_coef * vs[c]
    for k in range(nck):
        accel = gathered(2 + k)
        for c in range(2):
            own_bg[k, :, c] = accel[c]
            src[k, own, c] = ms[c] * accel[c]

    halo = 2 * BLOCK
    soon, rest = halo // 4, halo // 2

    def pairs(make):
        return make(0, lo_id), make(1, hi_id)

    def ranges(side, near_at, size):
        at = nz - near_at - size if side else near_at
        return pl.ds(nz + at, size), pl.ds(at if side else 2 * nz + at, size)

    def first_coefs(side, where):
        a, b = ranges(side, 0, soon)
        c, d = ranges(side, soon, soon)
        i = 3 * side
        j = 3 * (1 - side)
        return [
            remote(src.at[0, c], src.at[0, d], s_c.at[i], r_c.at[j], where),
            remote(src.at[:, a], src.at[:, b], s_c.at[i + 1], r_c.at[j + 1], where),
            remote(vel.at[a], vel.at[b], s_c.at[i + 2], r_c.at[j + 2], where),
        ]

    def later_coefs(side, where):
        a, b = ranges(side, soon, halo - soon)
        c, _ = ranges(side, 2 * soon, soon)
        d, _ = ranges(side, soon, rest)
        i = 6 + 3 * side
        j = 6 + 3 * (1 - side)
        return [
            remote(src.at[0, c], far.at[1 - side, 0, pl.ds(0, soon)], s_c.at[i], r_c.at[j], where),
            remote(src.at[pl.ds(1, nck - 1), d], far.at[1 - side, pl.ds(1, nck - 1)], s_c.at[i + 1], r_c.at[j + 1], where),
            remote(vel.at[a], vel.at[b], s_c.at[i + 2], r_c.at[j + 2], where),
        ]

    def newer_copies(e, newer):
        def make(side, where):
            a, b = ranges(side, 0, nz)
            return [remote(newer.at[a], newer.at[b], s_f.at[e, side, 0], r_f.at[e, 1 - side, 0], where)]
        return pairs(make)

    def older_copies(e, older):
        def make(side, where):
            a, b = ranges(side, 2, halo - 4)
            return [remote(older.at[a], older.at[b], s_f.at[e, side, 1], r_f.at[e, 1 - side, 1], where)]
        return pairs(make)

    def launch(copies):
        to_lo, to_hi = copies

        @pl.when(has_hi)
        def _():
            for c in to_hi:
                c.start()

        @pl.when(has_lo)
        def _():
            for c in to_lo:
                c.start()

    def settle(copies):
        to_lo, to_hi = copies

        @pl.when(has_hi)
        def _():
            for c in to_lo:
                c.wait_recv()
            for c in to_hi:
                c.wait_send()

        @pl.when(has_lo)
        def _():
            for c in to_hi:
                c.wait_recv()
            for c in to_lo:
                c.wait_send()

    opening, closing = pairs(first_coefs), pairs(later_coefs)
    launch(opening)
    launch(closing)

    def sent_in(c, carry):
        @pl.when(gz * per + c != pos)
        def _():
            remote(stage.at[c], arrival(my_row), s_in.at[c], r_in.at[my_row], lo_id).wait_send()

        return carry

    lax.fori_loop(0, per, sent_in, 0)
    settle(opening)

    def lateral_sums(ref, width):
        size = nz + 2 * width
        f = ref[pl.ds(nz - width, size)].reshape(size * rows, lanes)
        top = f.astype(jnp.bfloat16)
        low = (f - top.astype(f32)).astype(jnp.bfloat16)
        mixed[pl.ds((nz - width) * rows, size * rows)] = jnp.dot(
            jnp.concatenate([top, low], axis=1), taps[...], preferred_element_type=f32
        )

    def spread(ref, at, size):
        f = ref[pl.ds(at, size)]
        m = pl.ds(at * rows, size * rows)
        shape = (size, 2) + tile
        near = ref[pl.ds(at + 1, size)] + ref[pl.ds(at - 1, size)]
        wide = ref[pl.ds(at + 2, size)] + ref[pl.ds(at - 2, size)]
        flat = plane.lateral(f, mixed[m, 0:lanes].reshape(shape), mixed[m, lanes : 2 * lanes].reshape(shape))
        return flat + wide - 16.0 * near + 90.0 * f, f

    def groups(width):
        lo, hi = nz - width, 2 * nz + width
        for at in range(lo, hi, GROUP):
            yield at, min(GROUP, hi - at)

    def forward_step(t, width):
        k = ck_in[t]
        lateral_sums(hist.at[t - 1], width)
        for at, size in groups(width):
            here = pl.ds(at, size)
            lap, f = spread(hist.at[t - 1], at, size)
            value = 2.0 * f + vel[here] * lap + src[k, here]
            if t > 1:
                value = value - hist[t - 2, here]
            hist[t, here] = value

    def adjoint_step(t, width):
        k = ck_in[t]
        first = t == steps - 1
        if not first:
            for at, size in groups(width + 2):
                here = pl.ds(at, size)
                wbuf[here] = vel[here] * adj[t + 1, here]
            lateral_sums(wbuf, width)
        for at, size in groups(width):
            here = pl.ds(at, size)
            value = count[here] * hist[t, here]
            if not first:
                lap, _ = spread(wbuf, at, size)
                value = value + lap + 2.0 * adj[t + 1, here]
                if t < steps - 2:
                    value = value - adj[t + 2, here]
            adj[t, here] = value
        img[...] = img[...] + adj[t, nz : 2 * nz] * own_bg[k]

    blocks = steps // BLOCK

    for z in range(nz - 2 * soon, 2 * nz + 2 * soon):
        for c in range(2):
            hist[0, z, c] = src[0, z, c]
    forward_step(1, 2)
    older = older_copies(0, hist.at[1])
    launch(older)
    forward_step(2, 0)
    newer = newer_copies(0, hist.at[2])
    launch(newer)
    settle(closing)

    @pl.when(has_lo)
    def _():
        src[0, nz - halo + 2 : nz - halo + 2 + soon] = far[0, 0, 0:soon]
        src[1:, nz - halo + 2 : nz - soon] = far[0, 1:]

    @pl.when(has_hi)
    def _():
        src[0, 2 * nz + 2 * soon : 2 * nz + 3 * soon] = far[1, 0, 0:soon]
        src[1:, 2 * nz + soon : 2 * nz + 3 * soon] = far[1, 1:]

    settle(older)
    settle(newer)

    def forward_block(b):
        t = b * BLOCK - 1
        for j in range(BLOCK - 1):
            forward_step(t + j, halo - 2 * (j + 1))
        older = older_copies(b, hist.at[t + BLOCK - 2])
        launch(older)
        forward_step(t + BLOCK - 1, 0)
        newer = newer_copies(b, hist.at[t + BLOCK - 1])
        launch(newer)
        settle(older)
        settle(newer)

    for b in range(1, blocks):
        forward_block(b)

    def send_back(src_ref, dst, ss, rs, slot, g):
        def one(i, carry):
            row = lax.rem(my_row + rows // 2 + i, rows)
            other = (row != my_row) | (g != gz)
            piece = src_ref.at[pl.ds(pl.multiple_of(row * nz, nz), nz)]

            @pl.when(other)
            def _():
                remote(piece, dst.at[slot], ss.at[row], rs.at[slot], (row // gys, row % gys, g)).start()

            @pl.when(jnp.logical_not(other))
            def _():
                dst[slot] = piece[...]

            return carry

        lax.fori_loop(0, rows, one, 0)

    def sent_back(src_ref, dst, ss, rs, g):
        def one(row, carry):
            @pl.when((row != my_row) | (g != gz))
            def _():
                remote(src_ref.at[pl.ds(0, nz)], dst.at[0], ss.at[row], rs.at[0], lo_id).wait_send()

            return carry

        lax.fori_loop(0, rows, one, 0)

    def got_back(src_ref, dst, ss, rs, first, number):
        def one(c, carry):
            @pl.when(c + first != pos)
            def _():
                remote(src_ref.at[pl.ds(0, nz)], dst.at[c], ss.at[0], rs.at[c], lo_id).wait_recv()

            return carry

        lax.fori_loop(0, number, one, 0)

    near = 4
    apart = n // near
    team, seat = pos // near, pos % near

    def trace_sends(src_ref, dst, kind):
        number = near if kind == 0 else apart
        mine = seat if kind == 0 else team

        def one(i, carry):
            @pl.when(i != mine)
            def _():
                p = team * near + i if kind == 0 else i * near + seat
                remote(src_ref, dst.at[mine], s_t.at[kind, i], r_t.at[kind, mine], place_of(p, gxs, gys, gzs)).start()

            return carry

        lax.fori_loop(0, number, one, 0)

    def trace_waits(src_ref, dst, kind):
        number = near if kind == 0 else apart
        mine = seat if kind == 0 else team

        def one(i, carry):
            @pl.when(i != mine)
            def _():
                remote(src_ref, dst.at[i], s_t.at[kind, i], r_t.at[kind, i], lo_id).wait()

            return carry

        lax.fori_loop(0, number, one, 0)

    def gather_traces():
        picked = one_zr[nz * rows : 2 * nz * rows]
        lane_pick = one_lane.astype(jnp.bfloat16)
        lines = []
        for t in range(steps):
            table = hist[t, nz : 2 * nz].reshape(nz * rows, lanes)
            at_row = jnp.zeros((nz * rows, nrec), f32)
            for _ in range(3):
                piece = table.astype(jnp.bfloat16)
                at_row = at_row + jnp.dot(piece, lane_pick, preferred_element_type=f32)
                table = table - piece.astype(f32)
            lines.append(jnp.sum(at_row * picked, axis=0, keepdims=True))
        return jnp.concatenate(lines, axis=0)

    def give_back(field, dst):
        for g, value in enumerate(plane.split(field[:, 0], field[:, 1])):
            for z in range(nz):
                dst[pl.ds(g * nz + z, gxs, stride=gys * nz), :] = value[z]

    last = steps - 1
    forward_step(last, halo - 2)
    adjoint_step(last, halo - 2)
    adjoint_step(last - 1, halo - 4)
    adjoint_step(last - 2, halo - 6)
    older = older_copies(blocks, adj.at[last - 2])
    launch(older)
    adjoint_step(last - 3, 0)
    newer = newer_copies(blocks, adj.at[last - 3])
    launch(newer)
    give_back(hist[last, own], back_w)
    send_back(back_w, in_w, s_w, r_w, lax.rem(pos, per), owner)
    part[0] = gather_traces()
    tr1[seat] = part[0]
    trace_sends(part.at[0], tr1, 0)
    settle(older)
    settle(newer)

    def trace_relay():
        trace_waits(part.at[0], tr1, 0)
        total = tr1[0]
        for i in range(1, near):
            total = total + tr1[i]
        part[1] = total
        tr2[team] = total
        trace_sends(part.at[1], tr2, 1)

    def adjoint_block(b):
        t = last - BLOCK * b
        for j in range(BLOCK - 1):
            adjoint_step(t - j, halo - 2 * (j + 1))
        if b == blocks - 1:
            adjoint_step(t - BLOCK + 1, 0)
            return
        older = older_copies(blocks + b, adj.at[t - BLOCK + 2])
        launch(older)
        adjoint_step(t - BLOCK + 1, 0)
        newer = newer_copies(blocks + b, adj.at[t - BLOCK + 1])
        launch(newer)
        if b == 1:
            trace_relay()
        settle(older)
        settle(newer)

    for b in range(1, blocks):
        adjoint_block(b)

    give_back(img[...], back_i)
    send_back(back_i, in_i, s_i, r_i, lax.rem(pos, per), owner)
    trace_waits(part.at[1], tr2, 1)
    total = tr2[0]
    for i in range(1, apart):
        total = total + tr2[i]
    traces_ref[...] = total

    def put_out(buffer, out_ref):
        turned = buffer[...].reshape(sz, lanes).T
        for k in range(sx):
            out_ref[quarter_owner(k, gy)] = turned[k * sy : (k + 1) * sy]

    got_back(back_w, in_w, s_w, r_w, gz * per, per)
    put_out(in_w, wave_ref)
    sent_back(back_w, in_w, s_w, r_w, owner)
    sent_back(back_i, in_i, s_i, r_i, owner)

    got_back(back_i, in_i, s_i, r_i, gz * per, per)
    in_c[gz] = jnp.sum(in_i[...].reshape(sz, lanes), axis=0, keepdims=True)

    def sums_to(i, where):
        return remote(in_c.at[gz], in_c.at[gz], s_k.at[i], r_k.at[gz], (gx, gy, where))

    def sums_from(i):
        return remote(in_c.at[i], in_c.at[i], s_k.at[i], r_k.at[i], (gx, gy, i))

    for step in range(1, gzs):
        sums_to(step, lax.rem(gz + step, gzs)).start()
    put_out(in_i, image_ref)
    for step in range(1, gzs):
        sums_from(lax.rem(gz + step, gzs)).wait_recv()
    depth = in_c[0]
    for i in range(1, gzs):
        depth = depth + in_c[i]
    depth = depth / (sz * gzs)
    for k in range(sx):
        column_ref[pl.ds(quarter_owner(k, gy), 1), :] = depth[:, k * sy : (k + 1) * sy]
    for step in range(1, gzs):
        sums_to(step, lax.rem(gz + step, gzs)).wait_send()


def store_kernel(*refs):
    count = len(refs) // 2
    ins, outs, sems = refs[:count], refs[count : 2 * count], refs[2 * count]
    copies = [pltpu.make_async_copy(a, b, sems.at[i]) for i, (a, b) in enumerate(zip(ins, outs))]
    for copy in copies:
        copy.start()
    for copy in copies:
        copy.wait()


def chain_on_device(sizes, velocity_term, model_step, background, receivers, checkpoints):
    gxs, gys, gzs = sizes
    sx, sy, sz = model_step.shape
    nck, steps, nrec = background.shape[0], checkpoints.shape[0], receivers.shape[1]
    n, rows, lanes = gxs * gys * gzs, gxs * gys, sx * sy
    nz = sz * gzs // n
    per = sz // nz
    ext = 3 * nz
    blocks = steps // BLOCK
    halo = 2 * BLOCK
    dims = (gxs, gys, gzs, sx, sy, sz, nck, steps)
    f32 = jnp.float32
    dma = pltpu.SemaphoreType.DMA
    vmem = pl.BlockSpec(memory_space=pltpu.VMEM)
    hbm = pl.BlockSpec(memory_space=pltpu.HBM)
    tile = (2, gxs, lanes)
    shapes = (
        jax.ShapeDtypeStruct((sx, sy, sz), f32),
        jax.ShapeDtypeStruct((steps, nrec), f32),
        jax.ShapeDtypeStruct((sx, sy), f32),
        jax.ShapeDtypeStruct((sx, sy, sz), f32),
    )
    results = pl.pallas_call(
        functools.partial(chain_kernel, dims),
        out_shape=shapes,
        in_specs=[hbm] * 5,
        out_specs=(vmem,) * 4,
        scratch_shapes=[
            pltpu.VMEM(velocity_term.shape, f32),
            pltpu.VMEM(model_step.shape, f32),
            pltpu.VMEM(background.shape, background.dtype),
            pltpu.VMEM(receivers.shape, receivers.dtype),
            pltpu.SMEM(checkpoints.shape, checkpoints.dtype),
            pltpu.VMEM((per, (2 + nck) * nz, lanes), f32),
            pltpu.VMEM((rows * (2 + nck) * nz, lanes), f32),
            pltpu.VMEM((ext,) + tile, f32),
            pltpu.VMEM((nck, ext) + tile, f32),
            pltpu.VMEM((2, nck, halo // 2) + tile, f32),
            pltpu.VMEM((nck, nz) + tile, f32),
            pltpu.VMEM((steps, ext) + tile, f32),
            pltpu.VMEM((steps, ext) + tile, f32),
            pltpu.VMEM((ext,) + tile, f32),
            pltpu.VMEM((2 * lanes, 2 * lanes), jnp.bfloat16),
            pltpu.VMEM((ext * rows, 2 * lanes), f32),
            pltpu.VMEM((nz,) + tile, f32),
            pltpu.VMEM((ext,) + tile, f32),
            pltpu.VMEM((2, steps, nrec), f32),
            pltpu.VMEM((4, steps, nrec), f32),
            pltpu.VMEM((n // 4, steps, nrec), f32),
            pltpu.VMEM((rows * nz, lanes), f32),
            pltpu.VMEM((rows * nz, lanes), f32),
            pltpu.VMEM((per, nz, lanes), f32),
            pltpu.VMEM((per, nz, lanes), f32),
            pltpu.VMEM((gzs, 1, lanes), f32),
            dma((5,)),
            dma((per,)),
            dma((rows,)),
            dma((12,)),
            dma((12,)),
            dma((2 * blocks - 1, 2, 2)),
            dma((2 * blocks - 1, 2, 2)),
            dma((2, max(4, n // 4))),
            dma((2, max(4, n // 4))),
            dma((rows,)),
            dma((per,)),
            dma((rows,)),
            dma((per,)),
            dma((gzs,)),
            dma((gzs,)),
        ],
        compiler_params=pltpu.CompilerParams(
            collective_id=0, has_side_effects=True, vmem_limit_bytes=48 * 1024 * 1024
        ),
    )(*(
        pltpu.with_memory_space_constraint(a, pltpu.HBM)
        for a in (velocity_term, model_step, background, receivers, checkpoints)
    ))
    return pl.pallas_call(
        store_kernel,
        out_shape=shapes,
        in_specs=[vmem] * 4,
        out_specs=(hbm,) * 4,
        scratch_shapes=[dma((4,))],
        compiler_params=pltpu.CompilerParams(vmem_limit_bytes=1024 * 1024),
    )(*results)


def solution(mesh):
    gxs, gys, gzs = mesh.shape["gx"], mesh.shape["gy"], mesh.shape["gz"]
    n = gxs * gys * gzs

    def whole(velocity_term, model_step, background, receivers, checkpoints):
        nx, ny, depth = model_step.shape
        fits = (
            depth % (8 * n) == 0
            and depth // n == 2 * BLOCK
            and gxs == 8
            and gys == 2
            and n % 4 == 0
            and nx // gxs == 4
            and (nx // gxs) * (ny // gys) == 128
            and checkpoints.shape[0] == 4 * BLOCK
        )
        body = functools.partial(chain_on_device, (gxs, gys, gzs)) if fits else on_device
        return jax.shard_map(
            body,
            mesh=mesh,
            in_specs=(P("gx", "gy", "gz"), P("gx", "gy", "gz"), P(None, "gx", "gy", "gz"), P(), P()),
            out_specs=(P("gx", "gy", "gz"), P(), P("gx", "gy"), P("gx", "gy", "gz")),
            check_vma=False,
        )(velocity_term, model_step, background, receivers, checkpoints)

    return whole
```
